128 devices in a mesh: sub: 2 (over core), fsdp: 64 (over z, y, x).
Axes of the slice: x: 4, y: 4, z: 4, core: 2. Of those that a mesh axis runs over, the one named last changes fastest.
Arguments:
- x_in: bfloat16 [131072, 1024], P(('sub', 'fsdp'))
- w_up: bfloat16 [1, 1024, 4096], P(None, ('sub', 'fsdp'))
- w_down: bfloat16 [1, 4096, 1024], P(None, ('sub', 'fsdp'))
- grad_out: bfloat16 [131072, 1024], P(('sub', 'fsdp'))
Outputs:
- output 1: bfloat16 [131072, 1024], P(('sub', 'fsdp'))
- output 2: bfloat16 [131072, 1024], P(('sub', 'fsdp'))
- output 3: float32 [1, 1024, 4096], P(None, ('sub', 'fsdp'))
- output 4: float32 [1, 4096, 1024], P(None, ('sub', 'fsdp'))
All inputs are finite; a program needn't handle non-finite values.
Results may differ from the reference program's by a relative error of at most 0.001.
Values are sent between devices in bfloat16 or wider.
A program may use at most 1 GiB of HBM per device.

```python
import jax
import jax.numpy as jnp
from jax import lax

D = 1024
FF = 4096
LAYERS = 1
TOKENS_DEV = 1024
DEVICES = 128
TOKENS = TOKENS_DEV * DEVICES


def setup_inputs(seed: int = 0) -> dict:
    root_key = jax.random.key(seed)
    key_list = jax.random.split(root_key, 4)
    x_in = jax.random.normal(key_list[0], (TOKENS, D), jnp.float32).astype(jnp.bfloat16)
    w_up = (jax.random.normal(key_list[1], (LAYERS, D, FF), jnp.float32) * D ** -0.5).astype(jnp.bfloat16)
    w_down = (jax.random.normal(key_list[2], (LAYERS, FF, D), jnp.float32) * (FF * LAYERS) ** -0.5).astype(jnp.bfloat16)
    grad_out = jax.random.normal(key_list[3], (TOKENS, D), jnp.float32).astype(jnp.bfloat16)
    return {"x_in": x_in, "w_up": w_up, "w_down": w_down, "grad_out": grad_out}


def layer_forward(hidden, up_mat, down_mat):
    pre_act = jnp.dot(hidden, up_mat, preferred_element_type=jnp.float32)
    act_bf = jax.nn.gelu(pre_act).astype(jnp.bfloat16)
    branch = jnp.dot(act_bf, down_mat, preferred_element_type=jnp.float32)
    return (hidden.astype(jnp.float32) + branch).astype(jnp.bfloat16)


def block_pass(x_blk, g_blk, w_up, w_down):
    def fwd_step(hidden, step_items):
        return layer_forward(hidden, step_items[0], step_items[1]), hidden

    y_blk, layer_inputs = lax.scan(fwd_step, x_blk, (w_up, w_down))

    def bwd_step(grad_now, step_items):
        layer_in, up_mat, down_mat = step_items
        pre_act = jnp.dot(layer_in, up_mat, preferred_element_type=jnp.float32)
        act_f32, gelu_back = jax.vjp(jax.nn.gelu, pre_act)
        act_bf = act_f32.astype(jnp.bfloat16)
        d_act = jnp.dot(grad_now, down_mat.T, preferred_element_type=jnp.float32)
        d_pre = gelu_back(d_act)[0].astype(jnp.bfloat16)
        down_grad = jnp.dot(act_bf.T, grad_now, preferred_element_type=jnp.float32)
        up_grad = jnp.dot(layer_in.T, d_pre, preferred_element_type=jnp.float32)
        back_branch = jnp.dot(d_pre, up_mat.T, preferred_element_type=jnp.float32)
        new_grad = (grad_now.astype(jnp.float32) + back_branch).astype(jnp.bfloat16)
        return new_grad, (up_grad, down_grad)

    dx_blk, (up_grads, down_grads) = lax.scan(bwd_step, g_blk, (layer_inputs, w_up, w_down), reverse=True)
    return y_blk, dx_blk, up_grads, down_grads


def reference(x_in, w_up, w_down, grad_out):
    x_blocks = x_in.reshape(DEVICES, TOKENS_DEV, D)
    g_blocks = grad_out.reshape(DEVICES, TOKENS_DEV, D)

    def step(acc_pair, step_items):
        y_blk, dx_blk, up_grads, down_grads = block_pass(step_items[0], step_items[1], w_up, w_down)
        return (acc_pair[0] + up_grads, acc_pair[1] + down_grads), (y_blk, dx_blk)

    zero_acc = (jnp.zeros((LAYERS, D, FF), jnp.float32), jnp.zeros((LAYERS, FF, D), jnp.float32))
    (dw_up, dw_down), (y_blocks, dx_blocks) = lax.scan(step, zero_acc, (x_blocks, g_blocks))
    return y_blocks.reshape(TOKENS, D), dx_blocks.reshape(TOKENS, D), dw_up, dw_down
```

```python
import jax
import jax.numpy as jnp
from jax import lax
from jax.experimental import pallas as pl
from jax.experimental.pallas import tpu as pltpu
from jax.sharding import PartitionSpec as P

f32, bf16 = jnp.float32, jnp.bfloat16
MESH = pl.DeviceIdType.MESH
NN, NT, TN = [(((i,), (k,)), ((), ())) for i, k in ((1, 0), (1, 1), (0, 0))]
ANY = pl.BlockSpec(memory_space=pl.ANY)
VMEM = pl.BlockSpec(memory_space=pltpu.VMEM)
AXES = ("sub", "fsdp")

TOK = 1024
DIM = 1024
HALF = 2048
R = 4
SUBL, LANE = 8, 128
COL = 256
CHUNKS = HALF // COL
STEP = 512
STEPS = 2 * TOK // STEP
U2 = 16
SLOTS = 3
ROUNDS = (11, 11, 10)
CLASSES = DIMS = range(3)
PAIRS = ((0, 1), (2,))
BOTH = range(2)
ORDERS = ((0, 1, 2), (1, 2, 0), (2, 0, 1))
STRIDE = (R * R, R, 1)
C0 = 0.7978845608028654
C1 = 0.044715 * C0
ALL = slice(None)

W1_LANES = ((0, COL, 3), (3 * COL, COL, 3), (6 * COL, COL, 2))
W2_LANES = ((0, COL, 1), (COL, COL, 1), (2 * COL, 2 * COL, 1))


def dot(a, b, dims):
    return lax.dot_general(a, b, dims, preferred_element_type=f32)


def span(i, n):
    return pl.ds(pl.multiple_of(i * n, n), n)


class Place:
    def __init__(self):
        self.s, self.j = lax.axis_index("sub"), lax.axis_index("fsdp")
        self.c = [lax.rem(lax.div(self.j, n), R) for n in STRIDE]
        self.plus, self.minus, self.opp = [[lax.rem(c + o, R) for c in self.c] for o in (1, 3, 2)]
        self.partner = (1 - self.s, self.j)

    def dev(self, d, v):
        return (self.s, self.j + (v - self.c[d]) * STRIDE[d])

    def near(self, d, dirn):
        return self.minus[d] if dirn else self.plus[d]

    def others(self, d):
        return self.plus[d], self.minus[d], self.opp[d]


def remote(src, dst, ssem, rsem, dev):
    return pltpu.make_async_remote_copy(src, dst, ssem, rsem, device_id=dev, device_id_type=MESH)


def arrived(ref, sem):
    pltpu.make_async_copy(ref, ref, sem).wait()


def part(half, n=2):
    return ALL if half is None else pl.ds(half * n, n)


class Gather:
    def __init__(self, pc, w, lead, lanes, sems, base):
        self.pc, self.w, self.lead, self.lanes = pc, w, lead, lanes
        self.ssem, self.rsem = sems
        self.sbase, self.rbase = base
        self.subs = max(n for _, _, n in lanes)

    @staticmethod
    def counts(lanes):
        subs = max(n for _, _, n in lanes)
        return 1 + 3 * subs, 1 + 5 * subs

    def at(self, ln, changes):
        idx = list(self.pc.c)
        for d, v in changes:
            idx[d] = v
        return self.w.at[(*self.lead, *idx, ALL, ln)]

    def classes(self, i):
        return [k for k in CLASSES if i < self.lanes[k][2]]

    def stretch(self, k, i):
        lane0, width, subs = self.lanes[k]
        return pl.ds(lane0, width * subs) if i is None else pl.ds(lane0 + i * width, width)

    def wait(self, sem, n, i):
        lanes = sum(self.lanes[k][1] * (self.lanes[k][2] if i is None else 1) for k in self.classes(i or 0))
        box = [pl.ds(0, q) for q in n]
        ref = self.w.at[(*self.lead, *box, ALL, pl.ds(0, lanes))]
        arrived(ref, sem)

    def send(self, refs, ss, rs, d, v):
        for r in refs:
            remote(r, r, self.ssem.at[self.sbase + ss], self.rsem.at[self.rbase + rs], self.pc.dev(d, v)).start()

    def own_start(self):
        for k in CLASSES:
            d = ORDERS[k][0]
            for v in self.pc.others(d):
                self.send([self.at(self.stretch(k, None), ())], 0, 0, d, v)

    def own_end(self):
        self.wait(self.rsem.at[self.rbase], (3, 1, 1), None)

    def ring_start(self, i):
        for k in self.classes(i):
            d1, d, _ = ORDERS[k]
            for v in self.pc.others(d):
                self.send([self.at(self.stretch(k, i), ((d1, ALL),))], 1 + 3 * i, 1 + 5 * i, d, v)

    def ring_end(self, i):
        self.wait(self.rsem.at[self.rbase + 1 + 5 * i], (3, R, 1), i)

    def tree_refs(self, k, i, late, v, half):
        d1, d2, d3 = ORDERS[k]
        base = ((d1, part(half)), (d3, v))
        ln = self.stretch(k, i)
        return [self.at(ln, (*base, (d2, o))) for o in self.pc.others(d2)] if late else [self.at(ln, base)]

    def tree_start(self, i, late):
        for k in self.classes(i):
            d = ORDERS[k][2]
            for dirn in BOTH:
                refs = self.tree_refs(k, i, late, self.pc.c[d], None)
                self.send(refs, 2 + 3 * i + late, 2 + 5 * i + 2 * late, d, self.pc.near(d, dirn))

    def tree_mid(self, i, late):
        self.wait(self.rsem.at[self.rbase + 2 + 5 * i + 2 * late], (2, R, 3 if late else 1), i)
        for k in self.classes(i):
            d = ORDERS[k][2]
            for dirn in BOTH:
                refs = self.tree_refs(k, i, late, self.pc.near(d, 1 - dirn), dirn)
                self.send(refs, 2 + 3 * i + late, 3 + 5 * i + 2 * late, d, self.pc.near(d, dirn))

    def tree_end(self, i, late):
        self.wait(self.rsem.at[self.rbase + 3 + 5 * i + 2 * late], (1, R, 3 if late else 1), i)

    def drain(self):
        self.wait(self.ssem.at[self.sbase], (3, 1, 1), None)
        for i in range(self.subs):
            for q, n in enumerate(((3, R, 1), (3, R, 1), (3, R, 3))):
                self.wait(self.ssem.at[self.sbase + 1 + 3 * i + q], n, i)


class Scatter:
    def __init__(self, pc, pool, recv, sems, finish):
        self.pc, self.pool, self.recv, self.sems, self.finish = pc, pool, recv, sems, finish

    @staticmethod
    def place_of(u):
        v = u - U2
        return jnp.where(u < U2, 2 * U2 + u, R * lax.div(v, 2) + lax.rem(v, 2))

    def blk(self, u, k, ph, v, half):
        order = ORDERS[k]
        idx = [None] * len(order)
        for q in range(ph):
            idx[order[q]] = self.pc.c[order[q]]
        idx[order[ph]] = v
        free = [d for d in DIMS if idx[d] is None]
        for d in free:
            idx[d] = ALL
        lanes = ALL
        if free:
            idx[free[0]] = part(half)
        else:
            lanes = part(half, LANE)
        return self.pool.at[(self.place_of(u), *idx, ALL, lanes)]

    def landing(self, k, ph, slot, dirn, kind, half):
        r = self.recv[ph][kind].at[k, slot, dirn]
        if half is None or not kind:
            return r
        return r.at[part(half)] if ph < 2 else r.at[:, part(half, LANE)]

    def copy(self, n, k, ph, dirn, kind):
        d = ORDERS[k][ph]
        slot = lax.rem(n, SLOTS)
        near = self.pc.near(d, dirn)
        half = 1 - dirn if kind == 1 else dirn
        src = self.blk(n * 3 + k, k, ph, near if kind else self.pc.opp[d], half)
        dst = self.landing(k, ph, slot, dirn, min(kind, 1), half)
        return remote(src, dst, self.ssem(n, k // 2, ph), self.rsem(n, k // 2, ph, min(kind, 1)), self.pc.dev(d, near))

    def ssem(self, n, pair, ph):
        return self.sems[0].at[(ph * 2 + pair) * SLOTS + lax.rem(n, SLOTS)]

    def rsem(self, n, pair, ph, kind):
        return self.sems[1].at[((ph * 2 + pair) * 2 + kind) * SLOTS + lax.rem(n, SLOTS)]

    def received(self, n, pair, ph, kind):
        r, slot = self.recv[ph][kind], lax.rem(n, SLOTS)
        arrived(r.at[2, slot] if pair else r.at[pl.ds(0, 2), slot], self.rsem(n, pair, ph, kind))

    def sent(self, n, pair, ph):
        r = self.recv[ph][1]
        arrived(r.at[:, 0, 0] if pair else r.at[:, 0], self.ssem(n, pair, ph))

    def start(self, n, ks, ph):
        for kind in BOTH:
            for k in ks:
                for dirn in BOTH:
                    self.copy(n, k, ph, dirn, kind).start()

    def mid(self, n, ks, ph):
        self.received(n, ks[0] // 2, ph, 0)
        for k in ks:
            d = ORDERS[k][ph]
            for dirn in BOTH:
                b = self.blk(n * 3 + k, k, ph, self.pc.near(d, dirn), dirn)
                b[...] = b[...] + self.landing(k, ph, lax.rem(n, SLOTS), dirn, 0, None)[...]
        for k in ks:
            for dirn in BOTH:
                self.copy(n, k, ph, dirn, 2).start()

    def end(self, n, ks, ph):
        self.received(n, ks[0] // 2, ph, 1)
        for k in ks:
            own = self.blk(n * 3 + k, k, ph, self.pc.c[ORDERS[k][ph]], None)
            tot = own[...]
            for dirn in BOTH:
                tot = tot + self.landing(k, ph, lax.rem(n, SLOTS), dirn, 1, None)[...]
            if ph < 2:
                own[...] = tot
            else:
                self.finish(n * 3 + k, tot)
        self.sent(n, ks[0] // 2, ph)
        if ph < 2:
            self.start(n, ks, ph + 1)

    def each(self, n, fn):
        for ks in PAIRS:

            @pl.when((n >= 0) & (n < ROUNDS[ks[0]]))
            def _():
                fn(n, ks)

    def events(self, t):
        for ph in reversed(DIMS):
            self.each(t - 2 - 2 * ph, lambda n, ks: self.end(n, ks, ph))
            self.each(t - 1 - 2 * ph, lambda n, ks: self.mid(n, ks, ph))
        self.each(t, lambda n, ks: self.start(n, ks, 0))


def half_tanh(h, h2):
    return 0.5 * jnp.tanh(h * (C0 + C1 * h2))


def gelu(h):
    return h * (0.5 + half_tanh(h, h * h))


def gelu_slope(h):
    h2 = h * h
    t = half_tanh(h, h2)
    return (0.5 + t) + ((0.25 - t * t) * (2.0 * C0 + (6.0 * C1) * h2)) * h


def recv_shapes():
    out = []
    for ph in DIMS:
        lead, dims = (3, SLOTS, 2), [R] * (2 - ph)
        half = [2] + dims[1:] if dims else []
        out.append((*lead, *half, SUBL, COL if dims else LANE))
        out.append((*lead, *dims, SUBL, COL))
    return out


AG1, AG2 = Gather.counts(W1_LANES), Gather.counts(W2_LANES)
RS_SEMS = 3 * 2 * SLOTS
BLOCKS = DIM // COL


def kernel(xh, uph, dnh, gh, yo, gxo, dw1o, dw2o, landh, keeph, x, xt, g, w1, w2, a, pool, sb, dw1s, dw1l, *rest):
    recv, (ag_s, ag_r, rs_s, rs_r, lsem, xs, xr, spare_sem) = rest[:6], rest[6:]
    pc = Place()
    s = pc.s
    own, theirs = span(s, TOK), span(1 - s, TOK)
    my_lanes, their_lanes = span(s, HALF), span(1 - s, HALF)
    scope = jax.named_scope

    loads = [
        pltpu.make_async_copy(src, dst, lsem.at[i])
        for i, (src, dst) in enumerate((
            (uph.at[:, my_lanes], w1.at[(s, *pc.c)]),
            (dnh, w2.at[tuple(pc.c)]),
            (xh, x.at[own]),
            (gh, g.at[own]),
        ))
    ]
    for c in loads:
        c.start()

    with scope("bar"):
        bar = pltpu.get_barrier_semaphore()
        peers = [pc.partner] + [pc.dev(d, v) for d in DIMS for v in pc.others(d)]
        for dev in peers:
            pl.semaphore_signal(bar, inc=1, device_id=dev, device_id_type=MESH)
        pl.semaphore_wait(bar, len(peers))

    swaps = [
        remote(src, dst, xs.at[i], xr.at[i], pc.partner)
        for i, (src, dst) in enumerate((
            (uph.at[:, their_lanes], w1.at[(s, *pc.c)]),
            (xh, x.at[own]),
            (gh, g.at[own]),
        ))
    ]
    for c in swaps:
        c.start()

    g1 = Gather(pc, w1, (ALL,), W1_LANES, (ag_s, ag_r), (0, 0))
    g2 = Gather(pc, w2, (), W2_LANES, (ag_s, ag_r), AG1)

    w1f = w1.reshape(DIM, HALF)
    w2f = w2.reshape(HALF, DIM)
    units = pool.reshape(3 * U2, R * R * R, SUBL, COL)

    with scope("swapw"):
        loads[0].wait()
        swaps[0].wait_recv()
    g1.own_start()
    with scope("own"):
        g1.own_end()
    for i in range(3):
        g1.ring_start(i)
    for i in range(3):
        g1.tree_start(i, 0)
    loads[1].wait()
    g2.own_start()

    loads[2].wait()
    swaps[1].wait_recv()

    def turn(i, _):
        at = span(i, COL)
        xt[:, at] = x[at, :].T
        return 0

    with scope("turn"):
        lax.fori_loop(0, 2 * TOK // COL, turn, 0)

    def ring_done(i):
        with scope(f"ring{i}"):
            g1.ring_end(i)
        g1.tree_start(i, 1)

    ring_done(0)
    ring_done(1)
    with scope("early0"):
        g1.tree_mid(0, 0)
    with scope("late0"):
        g1.tree_mid(0, 1)
    with scope("early1"):
        g1.tree_mid(1, 0)
    ring_done(2)
    with scope("early2"):
        g1.tree_mid(2, 0)

    def rows(i):
        return slice(STEP * i, STEP * (i + 1))

    def flat(c, i):
        return units.at[R * c + i]

    def hidden_dot(c, i):
        sb[i % 2, :STEP] = dot(x[rows(i), :], w1f[:, span(c, COL)], NN)

    def hidden_act(c, i):
        h = sb[i % 2, :STEP]
        flat(c, i)[...] = h.reshape(STEP // SUBL, SUBL, COL)
        a[rows(i), span(c, COL)] = gelu(h).astype(bf16)

    def dhidden_dot(c, i):
        sb[i % 2, :STEP] = dot(g[rows(i), :], w2f[span(c, COL), :], NT)

    def dhidden_act(c, i):
        slope = gelu_slope(flat(c, i)[...].reshape(STEP, COL))
        a[rows(i), span(c, COL)] = (slope * sb[i % 2, :STEP]).astype(bf16)

    def grad1(c):
        r = dot(xt[...], a[:, span(c, COL)], NN)
        for p in BOTH:
            flat(c, p)[...] = r[rows(p)].reshape(STEP // SUBL, SUBL, COL)

    def chunk_steps(dot_step, act_step, c, after):
        for i in range(STEPS):
            if i + 1 < STEPS:
                dot_step(c, i + 1)
            else:
                dot_step(after, 0)
            act_step(c, i)

    def grad2(nb):
        def rows_of(c):
            r = dot(a[:, span(c, COL)], g[:, pl.ds(nb * 2 * COL, 2 * COL)], TN)
            for b in BOTH:
                rr = r[:, COL * b:COL * (b + 1)].reshape(SUBL, R, SUBL, COL)
                for q in range(R):
                    units[2 * U2 + R * (2 * nb + b) + q, span(c, SUBL)] = rr[:, q]

        def body(i, _):
            for q in range(R):
                rows_of(i * R + q)
            return 0

        lax.fori_loop(0, CHUNKS // R, body, 0)

    def product(at, nb, i):
        lanes = span(nb, COL)
        return dot(a[at, :], w1f[lanes, :], NT) if i else dot(a[at, :], w2f[:, lanes], NN)

    def out_block(nb, i):
        lanes = span(nb, COL)
        return pltpu.make_async_copy((x, g)[i].at[own, lanes], (yo, gxo)[i].at[:, lanes], lsem.at[R + BLOCKS * i + nb])

    def keep_y(n):
        return pltpu.make_async_copy(sb.at[lax.rem(n, 3)], keeph.at[n], lsem.at[12 + lax.rem(n, 3)])

    def give_y_block(nb):
        return remote(keeph.at[2 * nb], landh.at[nb], xs.at[3 + nb], xr.at[3 + nb], pc.partner)

    def kept(n):
        keep_y(n).wait()

        @pl.when(lax.rem(n, 2) == 0)
        def _():
            give_y_block(lax.div(n, 2)).start()

    def give_y(n):
        @pl.when(n > 2)
        def _():
            kept(n - 3)

        at = pl.ds(pl.multiple_of(TOK * jnp.where(lax.rem(n, 2) == 0, 1 - s, s), TOK), TOK)
        sb[lax.rem(n, 3)] = product(at, lax.div(n, 2), 0)
        keep_y(n).start()

    def finish_block(nb, i, at, part_sum):
        res, lanes = (x, g)[i], span(nb, COL)
        res[at, lanes] = (res[at, lanes].astype(f32) + part_sum).astype(bf16)

    def fetch_y(nb):
        return [pltpu.make_async_copy(src, sb.at[b], lsem.at[12 + b]) for b, src in enumerate((landh.at[nb], keeph.at[2 * nb + 1]))]

    def take_y(nb):
        give_y_block(nb).wait_recv()
        for c in fetch_y(nb):
            c.start()
        for c in fetch_y(nb):
            c.wait()

        def add(h, _):
            at = pl.ds(pl.multiple_of(TOK * s + COL * h, COL), COL)
            finish_block(nb, 0, at, sb[0, span(h, COL)] + sb[1, span(h, COL)])
            return 0

        lax.fori_loop(0, TOK // COL, add, 0)
        out_block(nb, 0).start()

    def spare(n):
        return units.at[pl.ds(R * n + 2, 2)]

    def give_gx_block(nb):
        return remote(spare(BLOCKS + nb), spare(nb), xs.at[3 + BLOCKS + nb], xr.at[3 + BLOCKS + nb], pc.partner)

    def give_gx(nb):
        spare(BLOCKS + nb)[...] = product(theirs, nb, 1).reshape(2, TOK // 2 // SUBL, SUBL, COL)
        give_gx_block(nb).start()

    def take_gx(nb):
        give_gx_block(nb).wait_recv()

        def add(h, _):
            at = pl.ds(pl.multiple_of(TOK * s + STEP * h, STEP), STEP)
            finish_block(nb, 1, at, product(at, nb, 1) + flat(nb, 2 + h)[...].reshape(STEP, COL))
            return 0

        lax.fori_loop(0, TOK // STEP, add, 0)
        out_block(nb, 1).start()

    def loop(n, fn):
        def body(i, _):
            fn(i)
            return 0

        lax.fori_loop(0, n, body, 0)

    def at(t, first, fn, last=None):
        @pl.when((t >= first) & (t <= (first if last is None else last)))
        def _():
            with scope(f"task{first}"):
                fn()

    def arrive(i):
        g1.tree_end(i, 0)
        g1.tree_end(i, 1)

    def w2_ring():
        g2.own_end()
        g2.ring_start(0)
        g2.tree_start(0, 0)

    def w2_late():
        g2.ring_end(0)
        g2.tree_start(0, 1)
        g2.tree_mid(0, 0)

    def chunk(q):
        return lax.div(q, 3) + 3 * lax.rem(q, 3)

    with scope("arrive"):
        arrive(0)
    hidden_dot(0, 0)

    def hidden_step(q):
        at(q, 0, lambda: g1.tree_mid(1, 1))
        at(q, 1, lambda: g1.tree_mid(2, 1))
        at(q, 1, w2_ring)
        at(q, 2, lambda: arrive(1))
        at(q, 5, lambda: arrive(2))
        at(q, 5, w2_late)
        with scope("hidden"):
            chunk_steps(hidden_dot, hidden_act, chunk(q), chunk(jnp.minimum(q + 1, CHUNKS - 1)))

    loop(CHUNKS, hidden_step)
    loads[3].wait()
    swaps[2].wait_recv()
    with scope("gradtwo"):
        grad2(0)
    with scope("w2mid"):
        g2.tree_mid(0, 1)

    def finish(u, tot):
        @pl.when(u < U2)
        def _():
            dw2o[span(lax.rem(u, R), SUBL), span(lax.div(u, R), COL)] = tot

        @pl.when(u >= U2)
        def _():
            v = u - U2
            dw1s[lax.rem(v, 2), :, span(lax.div(v, 2), COL)] = tot

    rs = Scatter(pc, pool, [recv[2 * ph:2 * ph + 2] for ph in DIMS], (rs_s, rs_r), finish)

    def slot(t, _):
        with scope("ev"):
            rs.events(t)

        def first_task():
            grad2(1)
            for i in BOTH:
                g2.tree_end(0, i)
            g1.drain()
            g2.drain()

        at(t, 0, first_task)
        at(t, 1, lambda: loop(BLOCKS, lambda i: give_y(BLOCKS * (t - 1) + i)), 2)

        def first_dot():
            for n in range(3):
                kept(2 * BLOCKS - 3 + n)
            dhidden_dot(0, 0)

        def dhidden(c):
            chunk_steps(dhidden_dot, dhidden_act, c, jnp.minimum(c + 1, CHUNKS - 1))
            grad1(c)

        at(t, 3, first_dot)
        at(t, 3, lambda: loop(2, lambda i: dhidden(2 * (t - 3) + i)), 6)
        at(t, 5, lambda: pl.semaphore_signal(spare_sem, inc=1, device_id=pc.partner, device_id_type=MESH))
        at(t, 7, lambda: pl.semaphore_wait(spare_sem, 1))
        at(t, 7, lambda: loop(BLOCKS, give_gx))
        at(t, 8, lambda: loop(2, lambda i: take_y(2 * (t - 8) + i)), 9)
        at(t, 10, lambda: loop(2, lambda i: take_gx(2 * (t - 10) + i)), 11)
        return 0

    lax.fori_loop(0, max(ROUNDS) + 6, slot, 0)

    with scope("last"):
        last = remote(dw1s.at[1 - s], dw1l, xs.at[11], xr.at[11], pc.partner)
        last.start()
        dw1o[:, my_lanes] = dw1s[s]
        for c in swaps:
            c.wait_send()
        for nb in range(BLOCKS):
            give_y_block(nb).wait_send()
            give_gx_block(nb).wait_send()
        for i in BOTH:
            for nb in range(BLOCKS):
                out_block(nb, i).wait()
        last.wait()
        dw1o[:, their_lanes] = dw1l[...]


def local_stack(x, up, down, g):
    shape = jax.ShapeDtypeStruct
    dma = pltpu.SemaphoreType.DMA
    bf = [(2 * TOK, DIM), (DIM, 2 * TOK), (2 * TOK, DIM), (2, R, R, R, SUBL, HALF), (R, R, R, HALF // R**3, DIM), (2 * TOK, HALF)]
    ff = [(3 * U2, R, R, R, SUBL, COL), (3, TOK, COL), (2, SUBL, HALF), (SUBL, HALF)] + recv_shapes()
    call = pl.pallas_call(
        kernel,
        out_shape=(
            shape(x.shape, bf16),
            shape(g.shape, bf16),
            shape(up.shape[1:], f32),
            shape(down.shape[1:], f32),
            shape((BLOCKS, TOK, COL), f32),
            shape((2 * BLOCKS, TOK, COL), f32),
        ),
        in_specs=[ANY] * 4,
        out_specs=(ANY, ANY, VMEM, VMEM, ANY, ANY),
        scratch_shapes=[pltpu.VMEM(q, bf16) for q in bf] + [pltpu.VMEM(q, f32) for q in ff]
        + [dma((n,)) for n in (AG1[0] + AG2[0], AG1[1] + AG2[1], RS_SEMS, 2 * RS_SEMS, 15, 12, 12)] + [pltpu.SemaphoreType.REGULAR],
        compiler_params=pltpu.CompilerParams(collective_id=0, has_side_effects=True, vmem_limit_bytes=67043328),
        name="stack",
    )
    y, gx, dw1, dw2 = call(x, up[0], down[0], g)[:4]
    return y, gx, dw1[None], dw2[None]


def solution(mesh):
    tok, mat = P(AXES, None), P(None, AXES, None)
    return jax.shard_map(local_stack, mesh=mesh, in_specs=(tok, mat, mat, tok), out_specs=(tok, tok, mat, mat), check_vma=False)
```

```python
import jax
import jax.numpy as jnp
from jax import lax
from jax.experimental import pallas as pl
from jax.experimental.pallas import tpu as pltpu
from jax.sharding import PartitionSpec as P

f32, bf16 = jnp.float32, jnp.bfloat16
MESH = pl.DeviceIdType.MESH
NN, NT, TN = [(((i,), (k,)), ((), ())) for i, k in ((1, 0), (1, 1), (0, 0))]
ANY = pl.BlockSpec(memory_space=pl.ANY)
VMEM = pl.BlockSpec(memory_space=pltpu.VMEM)
AXES = ("sub", "fsdp")

TOK = 1024
DIM = 1024
HALF = 2048
R = 4
SUBL = 8
COL = 256
CHUNKS = HALF // COL
STEP = 512
STEPS = 2 * TOK // STEP
U2 = 16
SLOTS = 4
ROUNDS = (11, 11, 10)
CLASSES = DIMS = range(3)
PAIRS = ((0, 1), (2,))
BOTH = range(2)
ORDERS = ((0, 1, 2), (1, 2, 0), (2, 0, 1))
STRIDE = (R * R, R, 1)
C0 = 0.7978845608028654
C1 = 0.044715 * C0
ALL = slice(None)

W1_LANES = ((0, COL, 3), (3 * COL, COL, 3), (6 * COL, COL, 2))
W2_LANES = ((0, 256, 1), (256, 384, 1), (640, 384, 1))


def dot(a, b, dims):
    return lax.dot_general(a, b, dims, preferred_element_type=f32)


def span(i, n):
    return pl.ds(pl.multiple_of(i * n, n), n)


class Place:
    def __init__(self):
        self.s, self.j = lax.axis_index("sub"), lax.axis_index("fsdp")
        self.c = [lax.rem(lax.div(self.j, n), R) for n in STRIDE]
        self.plus, self.minus, self.opp = [[lax.rem(c + o, R) for c in self.c] for o in (1, 3, 2)]
        self.partner = (1 - self.s, self.j)

    def dev(self, d, v):
        return (self.s, self.j + (v - self.c[d]) * STRIDE[d])

    def near(self, d, dirn):
        return self.minus[d] if dirn else self.plus[d]

    def others(self, d):
        return self.plus[d], self.minus[d], self.opp[d]


def remote(src, dst, ssem, rsem, dev):
    return pltpu.make_async_remote_copy(src, dst, ssem, rsem, device_id=dev, device_id_type=MESH)


def arrived(ref, sem):
    pltpu.make_async_copy(ref, ref, sem).wait()


def part(half):
    return ALL if half is None else pl.ds(2 * half, 2)


class Gather:
    def __init__(self, pc, w, lead, lanes, sems, base):
        self.pc, self.w, self.lead, self.lanes, self.sems, self.base = pc, w, lead, lanes, sems, base

    @staticmethod
    def count(lanes):
        return 1 + 3 * max(n for _, _, n in lanes)

    def at(self, ln, changes):
        idx = list(self.pc.c)
        for d, v in changes:
            idx[d] = v
        return self.w.at[(*self.lead, *idx, ALL, ln)]

    def classes(self, i):
        return [k for k in CLASSES if i < self.lanes[k][2]]

    def stretch(self, k, step, i):
        lane0, width, subs = self.lanes[k]
        return pl.ds(lane0 + i * width, width) if step else pl.ds(lane0, width * subs)

    def sem(self, q, step, i):
        return self.sems[q].at[self.base + (3 * i + step if step else 0)]

    def send(self, block, step, halves, i, d, v):
        remote(block, block, self.sem(0, step, i), self.sem(1, step + halves, i), self.pc.dev(d, v)).start()

    def start(self, step, i=0):
        for k in self.classes(i):
            block = self.at(self.stretch(k, step, i), [(d, ALL) for d in ORDERS[k][:step]])
            d = ORDERS[k][step]
            for v in self.pc.others(d)[:3 if step < 2 else 2]:
                self.send(block, step, 0, i, d, v)

    def mid(self, i=0):
        self.wait(1, 2, 0, i, 2)
        for k in self.classes(i):
            d1, d2, d = ORDERS[k]
            for dirn in BOTH:
                behind = self.pc.near(d, 1 - dirn)
                block = self.at(self.stretch(k, 2, i), ((d1, part(dirn)), (d2, ALL), (d, behind)))
                self.send(block, 2, 1, i, d, self.pc.near(d, dirn))

    def wait(self, q, step, halves, i, n):
        lanes = sum(self.lanes[k][1] * (1 if step else self.lanes[k][2]) for k in self.classes(i))
        box = [pl.ds(0, m) for m in (n, *[R] * step, *[1] * (2 - step))]
        arrived(self.w.at[(*self.lead, *box, ALL, pl.ds(0, lanes))], self.sem(q, step + halves, i))

    def end(self, step, i=0):
        if step < 2:
            self.wait(1, step, 0, i, 3)
        else:
            self.wait(1, step, 1, i, 1)

    def drain(self):
        self.wait(0, 0, 0, 0, 3)
        for i in range(max(n for _, _, n in self.lanes)):
            for step in (1, 2):
                self.wait(0, step, 0, i, 3)


class Scatter:
    def __init__(self, pc, pool, recv, sems, finish):
        self.pc, self.pool, self.recv, self.sems, self.finish = pc, pool, recv, sems, finish

    @staticmethod
    def place_of(u):
        v = u - U2
        return jnp.where(u < U2, 2 * U2 + u, R * lax.div(v, 2) + lax.rem(v, 2))

    def blk(self, u, k, ph, v, half):
        order = ORDERS[k]
        idx = [None] * len(order)
        for q in range(ph):
            idx[order[q]] = self.pc.c[order[q]]
        idx[order[ph]] = v
        free = [d for d in DIMS if idx[d] is None]
        for d in free:
            idx[d] = ALL
        if free:
            idx[free[0]] = part(half)
        return self.pool.at[(self.place_of(u), *idx)]

    def landing(self, k, ph, slot, dirn, kind, half):
        r = self.recv[ph][kind].at[k, slot, dirn]
        return r if half is None or not kind else r.at[part(half)]

    def ssem(self, n, pair, ph):
        return self.sems[0].at[(ph * 2 + pair) * SLOTS + lax.rem(n, SLOTS)]

    def rsem(self, n, pair, ph, kind):
        return self.sems[1].at[((ph * 2 + pair) * 2 + kind) * SLOTS + lax.rem(n, SLOTS)]

    def send(self, n, k, ph, src, dst, kind, v):
        pair = k // 2
        remote(src, dst, self.ssem(n, pair, ph), self.rsem(n, pair, ph, kind), self.pc.dev(ORDERS[k][ph], v)).start()

    def copy(self, n, k, ph, dirn, kind):
        d = ORDERS[k][ph]
        near = self.pc.near(d, dirn)
        half = 1 - dirn if kind == 1 else dirn
        src = self.blk(n * 3 + k, k, ph, near if kind else self.pc.opp[d], half)
        dst = self.landing(k, ph, lax.rem(n, SLOTS), dirn, min(kind, 1), half)
        self.send(n, k, ph, src, dst, min(kind, 1), near)

    def received(self, n, pair, ph, kind):
        r, slot = self.recv[ph][kind], lax.rem(n, SLOTS)
        arrived(r.at[2, slot] if pair else r.at[pl.ds(0, 2), slot], self.rsem(n, pair, ph, kind))

    def sent(self, n, pair, ph):
        r = self.recv[ph][1]
        if ph < 2:
            ref = r.at[:, 0, 0] if pair else r.at[:, 0]
        else:
            ref = r.at[2, 0] if pair else r.at[pl.ds(0, 2), 0]
        arrived(ref, self.ssem(n, pair, ph))

    def start(self, n, ks, ph):
        for kind in BOTH:
            for k in ks:
                for dirn in BOTH:
                    self.copy(n, k, ph, dirn, kind)

    def start_last(self, n, ks):
        for k in ks:
            for i, v in enumerate(self.pc.others(ORDERS[k][2])):
                self.send(n, k, 2, self.blk(n * 3 + k, k, 2, v, None), self.recv[2][1].at[k, lax.rem(n, SLOTS), i], 1, v)

    def mid(self, n, ks, ph):
        self.received(n, ks[0] // 2, ph, 0)
        for k in ks:
            d = ORDERS[k][ph]
            for dirn in BOTH:
                b = self.blk(n * 3 + k, k, ph, self.pc.near(d, dirn), dirn)
                b[...] = b[...] + self.landing(k, ph, lax.rem(n, SLOTS), dirn, 0, None)[...]
        for k in ks:
            for dirn in BOTH:
                self.copy(n, k, ph, dirn, 2)

    def end(self, n, ks, ph):
        self.received(n, ks[0] // 2, ph, 1)
        for k in ks:
            own = self.blk(n * 3 + k, k, ph, self.pc.c[ORDERS[k][ph]], None)
            tot = own[...]
            for i in range(3 if ph == 2 else 2):
                tot = tot + self.recv[ph][1].at[k, lax.rem(n, SLOTS), i][...]
            if ph < 2:
                own[...] = tot
            else:
                self.finish(n * 3 + k, tot)
        self.sent(n, ks[0] // 2, ph)
        if ph == 0:
            self.start(n, ks, 1)
        elif ph == 1:
            self.start_last(n, ks)

    def each(self, n, fn):
        for ks in PAIRS:

            @pl.when((n >= 0) & (n < ROUNDS[ks[0]]))
            def _():
                fn(n, ks)

    def events(self, t):
        self.each(t - 5, lambda n, ks: self.end(n, ks, 2))
        for ph in (1, 0):
            self.each(t - 2 - 2 * ph, lambda n, ks: self.end(n, ks, ph))
            self.each(t - 1 - 2 * ph, lambda n, ks: self.mid(n, ks, ph))
        self.begin(t + 1)

    def begin(self, n):
        self.each(n, lambda n, ks: self.start(n, ks, 0))


def half_tanh(h, h2):
    return 0.5 * jnp.tanh(h * (C0 + C1 * h2))


def gelu(h):
    return h * (0.5 + half_tanh(h, h * h))


def gelu_slope(h):
    h2 = h * h
    t = half_tanh(h, h2)
    return (0.5 + t) + ((0.25 - t * t) * (2.0 * C0 + (6.0 * C1) * h2)) * h


def recv_shapes():
    out = []
    for dims in ((R, R), (R,)):
        for q in ((2, *dims[1:]), dims):
            out.append((3, SLOTS, 2, *q, SUBL, COL))
    return out + [(3, SLOTS, 3, SUBL, COL)]


AG1, AG2 = Gather.count(W1_LANES), Gather.count(W2_LANES)
RS_SEMS = 3 * 2 * SLOTS
BLOCKS = DIM // COL


def kernel(xh, uph, dnh, gh, yo, gxo, dw1o, dw2o, landh, keeph, x, xt, g, w1, w2, a, pool, sb, dw1s, dw1l, *rest):
    recv, (ag_s, ag_r, rs_s, rs_r, lsem, xs, xr, spare_sem) = rest[:5], rest[5:]
    pc = Place()
    s = pc.s
    own, theirs = span(s, TOK), span(1 - s, TOK)
    my_lanes, their_lanes = span(s, HALF), span(1 - s, HALF)
    scope = jax.named_scope

    loads = [
        pltpu.make_async_copy(src, dst, lsem.at[i])
        for i, (src, dst) in enumerate((
            (uph.at[:, my_lanes], w1.at[(s, *pc.c)]),
            (dnh, w2.at[tuple(pc.c)]),
            (xh, x.at[own]),
            (gh, g.at[own]),
        ))
    ]
    for c in loads:
        c.start()

    with scope("bar"):
        bar = pltpu.get_barrier_semaphore()
        peers = [pc.partner] + [pc.dev(d, v) for d in DIMS for v in pc.others(d)]
        for dev in peers:
            pl.semaphore_signal(bar, inc=1, device_id=dev, device_id_type=MESH)
        pl.semaphore_wait(bar, len(peers))

    swaps = [
        remote(src, dst, xs.at[i], xr.at[i], pc.partner)
        for i, (src, dst) in enumerate((
            (uph.at[:, their_lanes], w1.at[(s, *pc.c)]),
            (xh, x.at[own]),
            (gh, g.at[own]),
        ))
    ]
    for c in swaps:
        c.start()

    g1 = Gather(pc, w1, (ALL,), W1_LANES, (ag_s, ag_r), 0)
    g2 = Gather(pc, w2, (), W2_LANES, (ag_s, ag_r), AG1)

    w1f = w1.reshape(DIM, HALF)
    w2f = w2.reshape(HALF, DIM)
    units = pool.reshape(3 * U2, R * R * R, SUBL, COL)

    with scope("swapw"):
        loads[0].wait()
        swaps[0].wait_recv()
    g1.start(0)
    loads[1].wait()
    g2.start(0)
    with scope("own"):
        g1.end(0)
    for i in range(3):
        g1.start(1, i)
    with scope("own2"):
        g2.end(0)
    g2.start(1)
    for i in BOTH:
        with scope("ring"):
            g1.end(1, i)
        g1.start(2, i)
    with scope("mid"):
        g1.mid(0)
    with scope("ring"):
        g1.end(1, 2)
    g1.start(2, 2)
    with scope("mid"):
        g1.mid(1)
    with scope("ring2"):
        g2.end(1)
    g2.start(2)

    def turn(i, _):
        at = span(i, COL)
        xt[:, at] = x[at, :].T
        return 0

    loads[2].wait()
    swaps[1].wait_recv()
    with scope("turn"):
        lax.fori_loop(0, 2 * TOK // COL, turn, 0)

    def rows(i):
        return slice(STEP * i, STEP * (i + 1))

    def flat(c, i):
        return units.at[R * c + i]

    def hidden_dot(c, i):
        sb[i % 2, :STEP] = dot(x[rows(i), :], w1f[:, span(c, COL)], NN)

    def hidden_act(c, i):
        h = sb[i % 2, :STEP]
        flat(c, i)[...] = h.reshape(STEP // SUBL, SUBL, COL)
        a[rows(i), span(c, COL)] = gelu(h).astype(bf16)

    def dhidden_dot(c, i):
        sb[i % 2, :STEP] = dot(g[rows(i), :], w2f[span(c, COL), :], NT)

    def dhidden_act(c, i):
        slope = gelu_slope(flat(c, i)[...].reshape(STEP, COL))
        a[rows(i), span(c, COL)] = (slope * sb[i % 2, :STEP]).astype(bf16)

    def grad1(c):
        r = dot(xt[...], a[:, span(c, COL)], NN)
        for p in BOTH:
            flat(c, p)[...] = r[rows(p)].reshape(STEP // SUBL, SUBL, COL)

    def chunk_steps(dot_step, act_step, c, after):
        for i in range(STEPS):
            if i + 1 < STEPS:
                dot_step(c, i + 1)
            else:
                dot_step(after, 0)
            act_step(c, i)

    def grad2_rows(c, nb):
        r = dot(a[:, span(c, COL)], g[:, pl.ds(nb * 2 * COL, 2 * COL)], TN)
        for b in BOTH:
            rr = r[:, COL * b:COL * (b + 1)].reshape(SUBL, R, SUBL, COL)
            for q in range(R):
                units[2 * U2 + R * (2 * nb + b) + q, span(c, SUBL)] = rr[:, q]

    def grad2(nb):
        def body(i, _):
            for q in range(R):
                grad2_rows(i * R + q, nb)
            return 0

        lax.fori_loop(0, CHUNKS // R, body, 0)

    def product(at, nb, i):
        lanes = span(nb, COL)
        return dot(a[at, :], w1f[lanes, :], NT) if i else dot(a[at, :], w2f[:, lanes], NN)

    def out_block(nb, i):
        lanes = span(nb, COL)
        return pltpu.make_async_copy((x, g)[i].at[own, lanes], (yo, gxo)[i].at[:, lanes], lsem.at[R + BLOCKS * i + nb])

    def keep_y(n):
        return pltpu.make_async_copy(sb.at[lax.rem(n, 3)], keeph.at[n], lsem.at[12 + lax.rem(n, 3)])

    def give_y_block(nb):
        return remote(keeph.at[2 * nb], landh.at[nb], xs.at[3 + nb], xr.at[3 + nb], pc.partner)

    def kept(n):
        keep_y(n).wait()

        @pl.when(lax.rem(n, 2) == 0)
        def _():
            give_y_block(lax.div(n, 2)).start()

    def give_y(n):
        @pl.when(n > 2)
        def _():
            kept(n - 3)

        at = pl.ds(pl.multiple_of(TOK * jnp.where(lax.rem(n, 2) == 0, 1 - s, s), TOK), TOK)
        sb[lax.rem(n, 3)] = product(at, lax.div(n, 2), 0)
        keep_y(n).start()

    def finish_block(nb, i, at, part_sum):
        res, lanes = (x, g)[i], span(nb, COL)
        res[at, lanes] = (res[at, lanes].astype(f32) + part_sum).astype(bf16)

    def fetched_y(nb):
        return [pltpu.make_async_copy(src, sb.at[b], lsem.at[12 + b]) for b, src in enumerate((landh.at[nb], keeph.at[2 * nb + 1]))]

    def fetch_y(nb):
        give_y_block(nb).wait_recv()
        for c in fetched_y(nb):
            c.start()

    def take_y(nb):
        for c in fetched_y(nb):
            c.wait()

        def add(h, _):
            at = pl.ds(pl.multiple_of(TOK * s + COL * h, COL), COL)
            finish_block(nb, 0, at, sb[0, span(h, COL)] + sb[1, span(h, COL)])
            return 0

        lax.fori_loop(0, TOK // COL, add, 0)
        out_block(nb, 0).start()

    def spare(n):
        return units.at[pl.ds(R * n + 2, 2)]

    def give_gx_block(nb):
        return remote(spare(BLOCKS + nb), spare(nb), xs.at[3 + BLOCKS + nb], xr.at[3 + BLOCKS + nb], pc.partner)

    def give_gx(nb):
        spare(BLOCKS + nb)[...] = product(theirs, nb, 1).reshape(2, TOK // 2 // SUBL, SUBL, COL)
        give_gx_block(nb).start()

    def take_gx(nb):
        give_gx_block(nb).wait_recv()

        def add(h, _):
            at = pl.ds(pl.multiple_of(TOK * s + STEP * h, STEP), STEP)
            finish_block(nb, 1, at, product(at, nb, 1) + flat(nb, 2 + h)[...].reshape(STEP, COL))
            return 0

        lax.fori_loop(0, TOK // STEP, add, 0)
        out_block(nb, 1).start()

    def loop(n, fn):
        def body(i, _):
            fn(i)
            return 0

        lax.fori_loop(0, n, body, 0)

    def at(t, first, fn, last=None):
        @pl.when((t >= first) & (t <= (first if last is None else last)))
        def _():
            with scope(f"task{first}"):
                fn()

    def columns(i, _):
        with scope("arrive"):
            for q in range(3):
                at(i, q, lambda q=q: g1.end(2, q))
        at(i, 2, g2.mid)
        n = jnp.where(i < 2, 3, 2)
        hidden_dot(i, 0)

        def step(q, _):
            at(3 * i + q, 2, lambda: g1.mid(2))
            chunk_steps(hidden_dot, hidden_act, i + 3 * q, i + 3 * jnp.minimum(q + 1, n - 1))
            return 0

        with scope("hidden"):
            lax.fori_loop(0, n, step, 0)
        with scope("gradtwo"):
            for last in (1, 2):

                @pl.when((i < 2) if last == 2 else (i == 2))
                def _():
                    for q in range(last + 1):
                        grad2_rows(i + 3 * q, 0)

        return 0

    loads[3].wait()
    swaps[2].wait_recv()
    lax.fori_loop(0, 3, columns, 0)

    def finish(u, tot):
        @pl.when(u < U2)
        def _():
            dw2o[span(lax.rem(u, R), SUBL), span(lax.div(u, R), COL)] = tot

        @pl.when(u >= U2)
        def _():
            v = u - U2
            dw1s[lax.rem(v, 2), :, span(lax.div(v, 2), COL)] = tot

    rs = Scatter(pc, pool, [recv[:2], recv[2:4], (None, recv[4])], (rs_s, rs_r), finish)

    def first_dot():
        for n in range(3):
            kept(2 * BLOCKS - 3 + n)
        dhidden_dot(0, 0)

    def dhidden(c):
        chunk_steps(dhidden_dot, dhidden_act, c, jnp.minimum(c + 1, CHUNKS - 1))
        grad1(c)

    def settle():
        g2.end(2)
        g1.drain()
        g2.drain()

    def chunks_before(t):
        return jnp.clip(2 * (t - 3), 0, CHUNKS)

    with scope("start"):
        rs.begin(jnp.int32(0))

    def slot(t, _):
        with scope("ev"):
            rs.events(t)

        at(t, 0, lambda: grad2(1))
        at(t, 0, settle)
        at(t, 1, lambda: loop(BLOCKS, lambda i: give_y(BLOCKS * (t - 1) + i)), 2)
        at(t, 3, first_dot)

        def more(c, _):
            with scope("dh"):
                dhidden(c)
            return 0

        lax.fori_loop(chunks_before(t), chunks_before(t + 1), more, 0)
        at(t, 5, lambda: pl.semaphore_signal(spare_sem, inc=1, device_id=pc.partner, device_id_type=MESH))
        at(t, 7, lambda: pl.semaphore_wait(spare_sem, 1))

        def tokens(nb):
            fetch_y(nb)
            give_gx(nb)
            take_y(nb)

        at(t, 7, lambda: loop(2, lambda i: tokens(2 * (t - 7) + i)), 8)
        at(t, 9, lambda: take_gx(t - 9), 12)
        return 0

    lax.fori_loop(0, max(ROUNDS) + 5, slot, 0)

    with scope("last"):
        last = remote(dw1s.at[1 - s], dw1l, xs.at[11], xr.at[11], pc.partner)
        last.start()
        dw1o[:, my_lanes] = dw1s[s]
        for c in swaps:
            c.wait_send()
        for nb in range(BLOCKS):
            give_y_block(nb).wait_send()
            give_gx_block(nb).wait_send()
        for i in BOTH:
            for nb in range(BLOCKS):
                out_block(nb, i).wait()
        last.wait()
        dw1o[:, their_lanes] = dw1l[...]


def copy_out(*refs):
    n = (len(refs) - 2) // 3
    src, dst, mid, (into, out) = refs[:n], refs[n:2 * n], refs[2 * n:3 * n], refs[3 * n:]
    pieces = []
    for refs_of in zip(src, mid, dst):
        rows = max(refs_of[0].shape[0] // 2, SUBL)
        pieces += [[q.at[pl.ds(h, rows)] for q in refs_of] for h in range(0, refs_of[0].shape[0], rows)]
    steps = [[pltpu.make_async_copy(p[e], p[e + 1], sem.at[i]) for e, sem in enumerate((into, out))] for i, p in enumerate(pieces)]
    for first, _ in steps:
        first.start()
    for first, second in steps:
        first.wait()
        second.start()
    for _, second in steps:
        second.wait()


def local_stack(x, up, down, g):
    shape = jax.ShapeDtypeStruct
    dma = pltpu.SemaphoreType.DMA
    bf = [(2 * TOK, DIM), (DIM, 2 * TOK), (2 * TOK, DIM), (2, R, R, R, SUBL, HALF), (R, R, R, HALF // R**3, DIM), (2 * TOK, HALF)]
    ff = [(3 * U2, R, R, R, SUBL, COL), (3, TOK, COL), (2, SUBL, HALF), (SUBL, HALF)] + recv_shapes()
    call = pl.pallas_call(
        kernel,
        out_shape=(
            shape(x.shape, bf16),
            shape(g.shape, bf16),
            shape(up.shape[1:], f32),
            shape(down.shape[1:], f32),
            shape((BLOCKS, TOK, COL), f32),
            shape((2 * BLOCKS, TOK, COL), f32),
        ),
        in_specs=[ANY] * 4,
        out_specs=(ANY, ANY, VMEM, VMEM, ANY, ANY),
        scratch_shapes=[pltpu.VMEM(q, bf16) for q in bf] + [pltpu.VMEM(q, f32) for q in ff]
        + [dma((n,)) for n in (AG1 + AG2, AG1 + AG2, RS_SEMS, 2 * RS_SEMS, 15, 12, 12)] + [pltpu.SemaphoreType.REGULAR],
        compiler_params=pltpu.CompilerParams(collective_id=0, has_side_effects=True, vmem_limit_bytes=67043328),
        name="stack",
    )
    res = call(x, up[0], down[0], g)[:4]
    y, gx, dw1, dw2 = pl.pallas_call(
        copy_out,
        out_shape=[shape(q.shape, q.dtype) for q in res],
        in_specs=[ANY] * 4,
        out_specs=[ANY] * 4,
        scratch_shapes=[pltpu.VMEM(q.shape, q.dtype) for q in res] + [dma((2 * 4,))] * 2,
        name="copy_out",
    )(*res)
    return y, gx, dw1[None], dw2[None]


def solution(mesh):
    tok, mat = P(AXES, None), P(None, AXES, None)
    return jax.shard_map(local_stack, mesh=mesh, in_specs=(tok, mat, mat, tok), out_specs=(tok, tok, mat, mat), check_vma=False)
```

```python
import jax
import jax.numpy as jnp
from jax import lax
from jax.experimental import pallas as pl
from jax.experimental.pallas import tpu as pltpu
from jax.sharding import PartitionSpec as P

f32, bf16 = jnp.float32, jnp.bfloat16
MESH = pl.DeviceIdType.MESH
NN, NT, TN = [(((i,), (k,)), ((), ())) for i, k in ((1, 0), (1, 1), (0, 0))]
ANY = pl.BlockSpec(memory_space=pl.ANY)
VMEM = pl.BlockSpec(memory_space=pltpu.VMEM)
AXES = ("sub", "fsdp")

TOK = 1024
DIM = 1024
HALF = 2048
R = 4
SUBL = 8
COL = 256
CHUNKS = HALF // COL
STEP = 512
STEPS = 2 * TOK // STEP
U2 = 16
SLOTS = (4, 5, 5)
FEW = 3
SENDS = 4
ROUNDS = (11, 11, 10)
SHORT = 10
CLASSES = DIMS = range(3)
PAIRS = ((0, 1), (2,))
BOTH = range(2)
ORDERS = ((0, 1, 2), (1, 2, 0), (2, 0, 1))
STRIDE = (R * R, R, 1)
C0 = 0.7978845608028654
C1 = 0.044715 * C0
ALL = slice(None)

W1_LANES = ((0, COL, 3), (3 * COL, COL, 3), (6 * COL, COL, 2))
W2_LANES = ((0, 256, 1), (256, 384, 1), (640, 384, 1))


def dot(a, b, dims):
    return lax.dot_general(a, b, dims, preferred_element_type=f32)


def span(i, n):
    return pl.ds(pl.multiple_of(i * n, n), n)


class Place:
    def __init__(self):
        self.s, self.j = lax.axis_index("sub"), lax.axis_index("fsdp")
        self.c = [lax.rem(lax.div(self.j, n), R) for n in STRIDE]
        self.plus, self.minus, self.opp = [[lax.rem(c + o, R) for c in self.c] for o in (1, 3, 2)]
        self.partner = (1 - self.s, self.j)

    def dev(self, d, v):
        return (self.s, self.j + (v - self.c[d]) * STRIDE[d])

    def near(self, d, dirn):
        return self.minus[d] if dirn else self.plus[d]

    def others(self, d):
        return self.plus[d], self.minus[d], self.opp[d]


def remote(src, dst, ssem, rsem, dev):
    return pltpu.make_async_remote_copy(src, dst, ssem, rsem, device_id=dev, device_id_type=MESH)


def arrived(ref, sem):
    pltpu.make_async_copy(ref, ref, sem).wait()


def part(half):
    return ALL if half is None else pl.ds(2 * half, 2)


class Gather:
    def __init__(self, pc, w, lead, lanes, sems, base):
        self.pc, self.w, self.lead, self.lanes, self.sems, self.base = pc, w, lead, lanes, sems, base

    @staticmethod
    def count(lanes):
        return 1 + 3 * max(n for _, _, n in lanes)

    def at(self, ln, changes):
        idx = list(self.pc.c)
        for d, v in changes:
            idx[d] = v
        return self.w.at[(*self.lead, *idx, ALL, ln)]

    def classes(self, i):
        return [k for k in CLASSES if i < self.lanes[k][2]]

    def stretch(self, k, step, i):
        lane0, width, subs = self.lanes[k]
        return pl.ds(lane0 + i * width, width) if step else pl.ds(lane0, width * subs)

    def sem(self, q, step, i):
        return self.sems[q].at[self.base + (3 * i + step if step else 0)]

    def send(self, block, step, halves, i, d, v):
        remote(block, block, self.sem(0, step, i), self.sem(1, step + halves, i), self.pc.dev(d, v)).start()

    def start(self, step, i=0):
        for k in self.classes(i):
            block = self.at(self.stretch(k, step, i), [(d, ALL) for d in ORDERS[k][:step]])
            d = ORDERS[k][step]
            for v in self.pc.others(d)[:3 if step < 2 else 2]:
                self.send(block, step, 0, i, d, v)

    def mid(self, i=0):
        self.wait(1, 2, 0, i, 2)
        for k in self.classes(i):
            d1, d2, d = ORDERS[k]
            for dirn in BOTH:
                behind = self.pc.near(d, 1 - dirn)
                block = self.at(self.stretch(k, 2, i), ((d1, part(dirn)), (d2, ALL), (d, behind)))
                self.send(block, 2, 1, i, d, self.pc.near(d, dirn))

    def wait(self, q, step, halves, i, n):
        lanes = sum(self.lanes[k][1] * (1 if step else self.lanes[k][2]) for k in self.classes(i))
        box = [pl.ds(0, m) for m in (n, *[R] * step, *[1] * (2 - step))]
        arrived(self.w.at[(*self.lead, *box, ALL, pl.ds(0, lanes))], self.sem(q, step + halves, i))

    def end(self, step, i=0):
        if step < 2:
            self.wait(1, step, 0, i, 3)
        else:
            self.wait(1, step, 1, i, 1)

    def drain(self):
        self.wait(0, 0, 0, 0, 3)
        for i in range(max(n for _, _, n in self.lanes)):
            for step in (1, 2):
                self.wait(0, step, 0, i, 3)


PLAN = (
    ("end", 2, 11, 11007233111),
    ("second_end", 1, 9, 11013252111),
    ("middle", 1, 6, 11113051400),
    ("end", 0, 3, 12114012511),
    ("mid", 0, 1, 11211311303),
    ("start", 0, 0, 10112221211),
)


def slots_of(first, later):
    out = [first]
    for digit in str(later)[1:]:
        out.append(out[-1] + int(digit))
    return out


PLAN = [(name, ph, slots_of(*when)) for name, ph, *when in PLAN]
LAST_SLOT = max(q for *_, slots in PLAN for q in slots)
GIVE_SLOTS = (13, 15, 17, 18)
TAKE_SLOTS = (20, 21, 22, 23)


class Scatter:
    def __init__(self, pc, pool, recv, sems, credit, finish):
        self.pc, self.pool, self.recv, self.sems, self.credit, self.finish = pc, pool, recv, sems, credit, finish

    @staticmethod
    def place_of(u):
        v = u - U2
        return jnp.where(u < U2, 2 * U2 + u, R * lax.div(v, 2) + lax.rem(v, 2))

    def blk(self, u, k, ph, v, half):
        order = ORDERS[k]
        idx = [None] * len(order)
        for q in range(ph):
            idx[order[q]] = self.pc.c[order[q]]
        idx[order[ph]] = v
        free = [d for d in DIMS if idx[d] is None]
        for d in free:
            idx[d] = ALL
        if free:
            idx[free[0]] = part(half)
        return self.pool.at[(self.place_of(u), *idx)]

    def landing(self, n, k, ph, dirn, kind, half):
        r = self.recv[ph][kind]
        r = r.at[k, lax.rem(n, r.shape[1]), dirn]
        return r if half is None or not kind else r.at[part(half)]

    def ssem(self, n, pair, ph):
        return self.sems[0].at[(ph * 2 + pair) * SENDS + lax.rem(n, SENDS)]

    def rsem(self, n, pair, ph, kind):
        return self.sems[1].at[4 * sum(SLOTS[:ph]) + (pair * 2 + kind) * SLOTS[ph] + lax.rem(n, SLOTS[ph])]

    def send(self, n, k, ph, src, dst, kind, v):
        pair = k // 2
        remote(src, dst, self.ssem(n, pair, ph), self.rsem(n, pair, ph, kind), self.pc.dev(ORDERS[k][ph], v)).start()

    def copy(self, n, k, ph, dirn, kind):
        d = ORDERS[k][ph]
        near = self.pc.near(d, dirn)
        half = 1 - dirn if kind == 1 else dirn
        src = self.blk(n * 3 + k, k, ph, near if kind else self.pc.opp[d], half)
        dst = self.landing(n, k, ph, dirn, min(kind, 1), half)
        self.send(n, k, ph, src, dst, min(kind, 1), near)

    def start_short(self, n, ks):
        slot = lax.rem(n, SLOTS[1])
        for k in ks:
            slots = [self.recv[1][1].at[k, slot, i] for i in BOTH] + [self.recv[3][0].at[k]]
            for v, dst in zip(self.pc.others(ORDERS[k][1]), slots):
                self.send(n, k, 1, self.blk(n * 3 + k, k, 1, v, None), dst, 1, v)

    def end_short(self, n, ks):
        slot = lax.rem(n, SLOTS[1])
        arrived(self.recv[1][1].at[:, slot], self.rsem(n, 0, 1, 1))
        for k in ks:
            own = self.blk(n * 3 + k, k, 1, self.pc.c[ORDERS[k][1]], None)
            tot = own[...] + self.recv[3][0].at[k][...]
            for i in BOTH:
                tot = tot + self.recv[1][1].at[k, slot, i][...]
            own[...] = tot
        self.sent(n, 0, 1)
        self.start_last(n, ks)

    def received(self, n, pair, ph, kind):
        r, slot = self.recv[ph][kind], 0
        arrived(r.at[2, slot] if pair else r.at[pl.ds(0, 2), slot], self.rsem(n, pair, ph, kind))

    def sent(self, n, pair, ph):
        r = self.recv[ph][1]
        if ph < 2:
            ref = r.at[:, 0, 0] if pair else r.at[:, 0]
        else:
            ref = r.at[2, 0] if pair else r.at[pl.ds(0, 2), 0]
        arrived(ref, self.ssem(n, pair, ph))

    def start(self, n, ks, ph):
        if ph == 0:

            @pl.when(n >= FEW)
            def _():
                for k in ks:
                    for dirn in BOTH:
                        pl.semaphore_wait(self.credit.at[2 * k + dirn], 1)

        for kind in BOTH:
            for k in ks:
                for dirn in BOTH:
                    self.copy(n, k, ph, dirn, kind)

    def give_credit(self, ks):
        for k in ks:
            d = ORDERS[k][0]
            for dirn in BOTH:
                to = self.pc.dev(d, self.pc.near(d, dirn))
                pl.semaphore_signal(self.credit.at[2 * k + 1 - dirn], inc=1, device_id=to, device_id_type=MESH)

    def start_last(self, n, ks):
        for k in ks:
            for i, v in enumerate(self.pc.others(ORDERS[k][2])):
                self.send(n, k, 2, self.blk(n * 3 + k, k, 2, v, None), self.recv[2][1].at[k, lax.rem(n, SLOTS[2]), i], 1, v)

    @staticmethod
    def choose(n, ks, usual, short):
        if len(ks) == 1:
            usual()
        else:
            pl.when(n < SHORT)(usual)
            pl.when(n >= SHORT)(short)

    def middle(self, n, ks, ph):
        self.choose(n, ks, lambda: self.mid(n, ks, ph), lambda: None)

    def second_end(self, n, ks, ph):
        self.choose(n, ks, lambda: self.end(n, ks, ph), lambda: self.end_short(n, ks))

    def mid(self, n, ks, ph):
        self.received(n, ks[0] // 2, ph, 0)
        for k in ks:
            d = ORDERS[k][ph]
            for dirn in BOTH:
                b = self.blk(n * 3 + k, k, ph, self.pc.near(d, dirn), dirn)
                b[...] = b[...] + self.landing(n, k, ph, dirn, 0, None)[...]
        for k in ks:
            for dirn in BOTH:
                self.copy(n, k, ph, dirn, 2)
        if ph == 0:
            pl.when(n == 0)(lambda: self.give_credit(ks))

    def end(self, n, ks, ph):
        self.received(n, ks[0] // 2, ph, 1)
        for k in ks:
            own = self.blk(n * 3 + k, k, ph, self.pc.c[ORDERS[k][ph]], None)
            tot = own[...]
            for i in range(3 if ph == 2 else 2):
                tot = tot + self.recv[ph][1].at[k, lax.rem(n, SLOTS[ph]), i][...]
            if ph < 2:
                own[...] = tot
            else:
                self.finish(n * 3 + k, tot)
        self.sent(n, ks[0] // 2, ph)
        if ph == 0:
            self.choose(n, ks, lambda: self.start(n, ks, 1), lambda: self.start_short(n, ks))

            pl.when(n + SLOTS[0] < ROUNDS[ks[0]])(lambda: self.give_credit(ks))
        elif ph == 1:
            self.start_last(n, ks)

    def events(self, t, come):
        out = []
        for (name, ph, slots), first in zip(PLAN, come):

            def step(n, _):
                for ks in PAIRS:

                    @pl.when(n < ROUNDS[ks[0]])
                    def _():
                        getattr(self, name)(n, ks, ph)

                return 0

            out.append(sum(jnp.where(t >= q, 1, 0) for q in slots))
            lax.fori_loop(first, out[-1], step, 0)
        return tuple(out)


def half_tanh(h, h2):
    return 0.5 * jnp.tanh(h * (C0 + C1 * h2))


def gelu(h):
    return h * (0.5 + half_tanh(h, h * h))


def gelu_slope(h):
    h2 = h * h
    t = half_tanh(h, h2)
    return (0.5 + t) + ((0.25 - t * t) * (2.0 * C0 + (6.0 * C1) * h2)) * h


def recv_shapes():
    out = []
    for ph, dims in enumerate(((R, R), (R,))):
        for q in ((2, *dims[1:]), dims):
            out.append((3, SLOTS[ph] if ph or q == dims else FEW, 2, *q, SUBL, COL))
    return out + [(3, SLOTS[2], 3, SUBL, COL), (2, R, SUBL, COL)]


AG1, AG2 = Gather.count(W1_LANES), Gather.count(W2_LANES)
BLOCKS = DIM // COL


def kernel(xh, uph, dnh, gh, y, gx, dw1o, dw2o, landh, keeph, xp, xt, gp, w1, w2, a, pool, sb, dw1s, *rest):
    recv, (ag_s, ag_r, rs_s, rs_r, lsem, xs, xr, spare_sem, credit) = rest[:6], rest[6:]
    pc = Place()
    s = pc.s
    my_lanes, their_lanes = span(s, HALF), span(1 - s, HALF)
    scope = jax.named_scope
    tokens_x, tokens_g = (y, xp), (gx, gp)

    loads = [
        pltpu.make_async_copy(src, dst, lsem.at[i])
        for i, (src, dst) in enumerate((
            (uph.at[:, my_lanes], w1.at[(s, *pc.c)]),
            (dnh, w2.at[tuple(pc.c)]),
            (xh, y),
            (gh, gx),
        ))
    ]
    for c in loads:
        c.start()

    with scope("bar"):
        bar = pltpu.get_barrier_semaphore()
        peers = [pc.partner] + [pc.dev(d, v) for d in DIMS for v in pc.others(d)]
        for dev in peers:
            pl.semaphore_signal(bar, inc=1, device_id=dev, device_id_type=MESH)
        pl.semaphore_wait(bar, len(peers))

    swaps = [
        remote(src, dst, xs.at[i], xr.at[i], pc.partner)
        for i, (src, dst) in enumerate((
            (uph.at[:, their_lanes], w1.at[(s, *pc.c)]),
            (xh, xp),
            (gh, gp),
        ))
    ]
    for c in swaps:
        c.start()

    g1 = Gather(pc, w1, (ALL,), W1_LANES, (ag_s, ag_r), 0)
    g2 = Gather(pc, w2, (), W2_LANES, (ag_s, ag_r), AG1)

    w1f = w1.reshape(DIM, HALF)
    w2f = w2.reshape(HALF, DIM)
    units = pool.reshape(3 * U2, R * R * R, SUBL, COL)

    with scope("swapw"):
        loads[0].wait()
        swaps[0].wait_recv()
    g1.start(0)
    loads[1].wait()
    g2.start(0)
    with scope("own"):
        g1.end(0)
    for i in range(3):
        g1.start(1, i)
    with scope("own2"):
        g2.end(0)
    g2.start(1)
    for i in BOTH:
        with scope("ring"):
            g1.end(1, i)
        g1.start(2, i)
    with scope("mid"):
        g1.mid(0)
    with scope("ring"):
        g1.end(1, 2)
    g1.start(2, 2)
    with scope("mid"):
        g1.mid(1)
    with scope("ring2"):
        g2.end(1)
    g2.start(2)

    def turn(i, _):
        for q, part_x in enumerate(tokens_x):
            xt[:, pl.ds(pl.multiple_of(q * TOK + i * COL, COL), COL)] = part_x[span(i, COL), :].T
        return 0

    loads[2].wait()
    swaps[1].wait_recv()
    with scope("turn"):
        lax.fori_loop(0, TOK // COL, turn, 0)

    def rows(i):
        return slice(STEP * i, STEP * (i + 1))

    def step_of(pair, i):
        return pair[i // 2][rows(i % 2), :]

    def flat(c, i):
        return units.at[R * c + i]

    def hidden_dot(c, i):
        sb[i % 2, :STEP] = dot(step_of(tokens_x, i), w1f[:, span(c, COL)], NN)

    def hidden_act(c, i):
        h = sb[i % 2, :STEP]
        flat(c, i)[...] = h.reshape(STEP // SUBL, SUBL, COL)
        a[rows(i), span(c, COL)] = gelu(h).astype(bf16)

    def dhidden_dot(c, i):
        sb[i % 2, :STEP] = dot(step_of(tokens_g, i), w2f[span(c, COL), :], NT)

    def dhidden_act(c, i):
        slope = gelu_slope(flat(c, i)[...].reshape(STEP, COL))
        a[rows(i), span(c, COL)] = (slope * sb[i % 2, :STEP]).astype(bf16)

    def grad1(c):
        r = dot(xt[...], a[:, span(c, COL)], NN)
        for p in BOTH:
            flat(c, p)[...] = r[rows(p)].reshape(STEP // SUBL, SUBL, COL)

    def chunk_steps(dot_step, act_step, c, after):
        for i in range(STEPS):
            if i + 1 < STEPS:
                dot_step(c, i + 1)
            else:
                dot_step(after, 0)
            act_step(c, i)

    def grad2_rows(c, nb):
        cols = pl.ds(nb * 2 * COL, 2 * COL)
        both = jnp.concatenate([q[:, cols] for q in tokens_g])
        r = dot(a[:, span(c, COL)], both, TN)
        for b in BOTH:
            rr = r[:, COL * b:COL * (b + 1)].reshape(SUBL, R, SUBL, COL)
            for q in range(R):
                units[2 * U2 + R * (2 * nb + b) + q, span(c, SUBL)] = rr[:, q]

    def grad2_half(i, nb):
        for q in range(R):
            grad2_rows(i * R + q, nb)

    own, theirs = pl.ds(0, TOK), pl.ds(TOK, TOK)

    def product(at, nb, i):
        lanes = span(nb, COL)
        return dot(a[at, :], w1f[lanes, :], NT) if i else dot(a[at, :], w2f[:, lanes], NN)

    def keep_y(n):
        return pltpu.make_async_copy(sb.at[lax.rem(n, 3)], keeph.at[n], lsem.at[R + lax.rem(n, 3)])

    def give_y_block(nb):
        return remote(keeph.at[2 * nb], landh.at[nb], xs.at[3 + nb], xr.at[3 + nb], pc.partner)

    def kept(n):
        keep_y(n).wait()

        @pl.when(lax.rem(n, 2) == 0)
        def _():
            give_y_block(lax.div(n, 2)).start()

    def give_y(n):
        @pl.when(n > 2)
        def _():
            kept(n - 3)

        at = span(1 - lax.rem(n, 2), TOK)
        sb[lax.rem(n, 3)] = product(at, lax.div(n, 2), 0)
        keep_y(n).start()

    def finish_block(nb, res, at, part_sum):
        lanes = span(nb, COL)
        res[at, lanes] = (res[at, lanes].astype(f32) + part_sum).astype(bf16)

    def fetched_y(nb):
        return [pltpu.make_async_copy(src, sb.at[b], lsem.at[R + b]) for b, src in enumerate((landh.at[nb], keeph.at[2 * nb + 1]))]

    def fetch_y(nb):
        give_y_block(nb).wait_recv()
        for c in fetched_y(nb):
            c.start()

    def take_y(nb):
        for c in fetched_y(nb):
            c.wait()

        def add(h, _):
            finish_block(nb, y, span(h, COL), sb[0, span(h, COL)] + sb[1, span(h, COL)])
            return 0

        lax.fori_loop(0, TOK // COL, add, 0)

    def spare(n):
        return units.at[pl.ds(R * n + 2, 2)]

    def give_gx_block(nb):
        return remote(spare(BLOCKS + nb), spare(nb), xs.at[3 + BLOCKS + nb], xr.at[3 + BLOCKS + nb], pc.partner)

    def give_gx(nb):
        spare(BLOCKS + nb)[...] = product(theirs, nb, 1).reshape(2, TOK // 2 // SUBL, SUBL, COL)
        give_gx_block(nb).start()

    def take_gx(nb):
        give_gx_block(nb).wait_recv()

        def add(h, _):
            at = span(h, STEP)
            finish_block(nb, gx, at, product(at, nb, 1) + flat(nb, 2 + h)[...].reshape(STEP, COL))
            return 0

        lax.fori_loop(0, TOK // STEP, add, 0)

    def loop(n, fn):
        def body(i, _):
            fn(i)
            return 0

        lax.fori_loop(0, n, body, 0)

    def at(t, first, fn, last=None):
        @pl.when((t >= first) & (t <= (first if last is None else last)))
        def _():
            with scope(f"task{first}"):
                fn()

    def columns(i, _):
        with scope("arrive"):
            for q in range(3):
                at(i, q, lambda q=q: g1.end(2, q))
        at(i, 2, g2.mid)
        n = jnp.where(i < 2, 3, 2)
        hidden_dot(i, 0)

        def step(q, _):
            at(3 * i + q, 2, lambda: g1.mid(2))
            chunk_steps(hidden_dot, hidden_act, i + 3 * q, i + 3 * jnp.minimum(q + 1, n - 1))
            return 0

        with scope("hidden"):
            lax.fori_loop(0, n, step, 0)
        with scope("gradtwo"):
            for last in (1, 2):

                @pl.when((i < 2) if last == 2 else (i == 2))
                def _():
                    for q in range(last + 1):
                        grad2_rows(i + 3 * q, 0)

        return 0

    loads[3].wait()
    swaps[2].wait_recv()
    lax.fori_loop(0, 3, columns, 0)

    def finish(u, tot):
        @pl.when(u < U2)
        def _():
            dw2o[span(lax.rem(u, R), SUBL), span(lax.div(u, R), COL)] = tot

        @pl.when(u >= U2)
        def _():
            v = u - U2
            q = lax.div(v, 2)

            @pl.when(lax.rem(v, 2) == s)
            def _():
                dw1o[:, pl.ds(pl.multiple_of(HALF * s + COL * q, COL), COL)] = tot

            @pl.when(lax.rem(v, 2) != s)
            def _():
                dw1s[:, span(q, COL)] = tot

    rs = Scatter(pc, pool, [recv[:2], recv[2:4], (None, recv[4]), recv[5:]], (rs_s, rs_r), credit, finish)

    def first_dot():
        for n in range(3):
            kept(2 * BLOCKS - 3 + n)
        dhidden_dot(0, 0)

    def dhidden(c):
        chunk_steps(dhidden_dot, dhidden_act, c, jnp.minimum(c + 1, CHUNKS - 1))
        grad1(c)

    def settle():
        g2.end(2)
        g1.drain()
        g2.drain()

    def slot(t, come):
        with scope("ev"):
            come = rs.events(t, come)

        at(t, 0, lambda: loop(2, lambda i: grad2_half(i, 1)))
        at(t, 1, settle)
        at(t, 1, lambda: loop(2, lambda i: give_y(2 * (t - 1) + i)), 4)
        at(t, 5, first_dot)
        at(t, 5, lambda: dhidden(t - 5), 12)
        at(t, 9, lambda: pl.semaphore_signal(spare_sem, inc=1, device_id=pc.partner, device_id_type=MESH))
        at(t, GIVE_SLOTS[0], lambda: pl.semaphore_wait(spare_sem, 1))

        def tokens(nb):
            fetch_y(nb)
            give_gx(nb)
            take_y(nb)

        for slots, task in ((GIVE_SLOTS, tokens), (TAKE_SLOTS, take_gx)):
            done = sum(jnp.where(t > q, 1, 0) for q in slots)
            lax.fori_loop(done, sum(jnp.where(t >= q, 1, 0) for q in slots), lambda nb, _, task=task: task(nb) or 0, 0)

        return come

    lax.fori_loop(0, LAST_SLOT + 1, slot, (jnp.int32(0),) * len(PLAN))

    with scope("last"):
        last = remote(dw1s, dw1o.at[:, my_lanes], xs.at[11], xr.at[11], pc.partner)
        last.start()
        for c in swaps:
            c.wait_send()
        for nb in range(BLOCKS):
            give_y_block(nb).wait_send()
            give_gx_block(nb).wait_send()
        last.wait()


def copy_out(*refs):
    n = len(refs) // 2
    copies = [pltpu.make_async_copy(src, dst, refs[-1].at[i]) for i, (src, dst) in enumerate(zip(refs[:n], refs[n:]))]
    for c in copies:
        c.start()
    for c in copies:
        c.wait()


def local_stack(x, up, down, g):
    shape = jax.ShapeDtypeStruct
    dma = pltpu.SemaphoreType.DMA
    bf = [(TOK, DIM), (DIM, 2 * TOK), (TOK, DIM), (2, R, R, R, SUBL, HALF), (R, R, R, HALF // R**3, DIM), (2 * TOK, HALF)]
    ff = [(3 * U2, R, R, R, SUBL, COL), (3, TOK, COL), (SUBL, HALF)] + recv_shapes()
    results = [(x.shape, bf16), (g.shape, bf16), (up.shape[1:], f32), (down.shape[1:], f32)]
    res = pl.pallas_call(
        kernel,
        out_shape=[pltpu.VMEM(*q) for q in results] + [shape((n, TOK, COL), f32) for n in (BLOCKS, 2 * BLOCKS)],
        in_specs=[ANY] * 4,
        out_specs=[VMEM] * 4 + [ANY] * 2,
        scratch_shapes=[pltpu.VMEM(q, bf16) for q in bf] + [pltpu.VMEM(q, f32) for q in ff]
        + [dma((n,)) for n in (AG1 + AG2, AG1 + AG2, 6 * SENDS, 4 * sum(SLOTS), 7, 12, 12)]
        + [pltpu.SemaphoreType.REGULAR, pltpu.SemaphoreType.REGULAR((6,))],
        compiler_params=pltpu.CompilerParams(collective_id=0, has_side_effects=True, vmem_limit_bytes=62586880),
        name="stack",
    )(x, up[0], down[0], g)[:4]
    y, gx, dw1, dw2 = pl.pallas_call(
        copy_out,
        out_shape=[shape(*q) for q in results],
        in_specs=[VMEM] * 4,
        out_specs=[ANY] * 4,
        scratch_shapes=[dma((4,))],
        compiler_params=pltpu.CompilerParams(vmem_limit_bytes=2**23),
        name="copy_out",
    )(*res)
    return y, gx, dw1[None], dw2[None]


def solution(mesh):
    tok, mat = P(AXES, None), P(None, AXES, None)
    return jax.shard_map(local_stack, mesh=mesh, in_specs=(tok, mat, mat, tok), out_specs=(tok, tok, mat, mat), check_vma=False)
```

```python
import jax
import jax.numpy as jnp
from jax import lax
from jax.experimental import pallas as pl
from jax.experimental.pallas import tpu as pltpu
from jax.sharding import PartitionSpec as P

f32, bf16 = jnp.float32, jnp.bfloat16
MESH = pl.DeviceIdType.MESH
NN, NT, TN = [(((i,), (k,)), ((), ())) for i, k in ((1, 0), (1, 1), (0, 0))]
ANY = pl.BlockSpec(memory_space=pl.ANY)
VMEM = pl.BlockSpec(memory_space=pltpu.VMEM)
AXES = ("sub", "fsdp")

TOK = 1024
DIM = 1024
HALF = 2048
R = 4
SUBL, LANES = 8, 128
COL = 256
CHUNKS = HALF // COL
STEP = 512
STEPS = 2 * TOK // STEP
U2 = 16
SLOTS = (4, 5, 5)
FEW = 3
SENDS = 4
ROUNDS = (11, 11, 10)
SHORT = 10
CLASSES = DIMS = range(3)
PAIRS = ((0, 1), (2,))
BOTH = range(2)
ORDERS = ((0, 1, 2), (1, 2, 0), (2, 0, 1))
STRIDE = (R * R, R, 1)
C0 = 0.7978845608028654
C1 = 0.044715 * C0
ALL = slice(None)

W1_LANES = ((0, COL, 3), (3 * COL, COL, 3), (6 * COL, COL, 2))
W2_LANES = ((0, LANES, 2), (2 * LANES, LANES, 3), (5 * LANES, LANES, 3))


def dot(a, b, dims):
    return lax.dot_general(a, b, dims, preferred_element_type=f32)


def span(i, n):
    return pl.ds(pl.multiple_of(i * n, n), n)


class Place:
    def __init__(self):
        self.s, self.j = lax.axis_index("sub"), lax.axis_index("fsdp")
        self.c = [lax.rem(lax.div(self.j, n), R) for n in STRIDE]
        self.plus, self.minus, self.opp = [[lax.rem(c + o, R) for c in self.c] for o in (1, 3, 2)]
        self.partner = (1 - self.s, self.j)

    def dev(self, d, v):
        return (self.s, self.j + (v - self.c[d]) * STRIDE[d])

    def near(self, d, dirn):
        return self.minus[d] if dirn else self.plus[d]

    def others(self, d):
        return self.plus[d], self.minus[d], self.opp[d]


def remote(src, dst, ssem, rsem, dev):
    return pltpu.make_async_remote_copy(src, dst, ssem, rsem, device_id=dev, device_id_type=MESH)


def arrived(ref, sem):
    pltpu.make_async_copy(ref, ref, sem).wait()


def part(half):
    return ALL if half is None else pl.ds(2 * half, 2)


class Gather:
    OWN, EARLY, RING, PLANE, HALVES = range(5)

    def __init__(self, pc, w, lead, lanes, sems, base):
        self.pc, self.w, self.lead, self.lanes, self.sems, self.base = pc, w, lead, lanes, sems, base

    @staticmethod
    def count(lanes):
        return 2 + 3 * max(n for _, _, n in lanes)

    def at(self, ln, changes):
        idx = list(self.pc.c)
        for d, v in changes:
            idx[d] = v
        return self.w.at[(*self.lead, *idx, ALL, ln)]

    def classes(self, i):
        return [k for k in CLASSES if i < self.lanes[k][2]]

    def stretch(self, k, step, i):
        lane0, width, subs = self.lanes[k]
        return pl.ds(lane0, width * subs) if step < self.RING else pl.ds(lane0 + i * width, width)

    def sem(self, q, step, i):
        return self.sems[q].at[self.base + step + 3 * i]

    def send(self, block, step, into, i, d, v):
        remote(block, block, self.sem(0, step, i), self.sem(1, into, i), self.pc.dev(d, v)).start()

    def start(self, step, i=0):
        for k in self.classes(i):
            ln = self.stretch(k, step, i)
            d1, d2, d3 = ORDERS[k]
            d = (d1, d2, d2, d3)[step]
            if step < self.RING:
                blocks = [self.at(ln, ())]
            elif step == self.RING:
                blocks = [self.at(ln, ((d1, v),)) for v in self.pc.others(d1)]
            else:
                blocks = [self.at(ln, ((d1, ALL), (d2, ALL)))]
            for v in self.pc.others(d)[:3 if step < self.PLANE else 2]:
                for block in blocks:
                    self.send(block, step, step, i, d, v)

    def mid(self, i=0):
        self.wait(1, self.PLANE, (2, R, R), i)
        for k in self.classes(i):
            d1, d2, d = ORDERS[k]
            for dirn in BOTH:
                behind = self.pc.near(d, 1 - dirn)
                block = self.at(self.stretch(k, self.PLANE, i), ((d1, part(dirn)), (d2, ALL), (d, behind)))
                self.send(block, self.PLANE, self.HALVES, i, d, self.pc.near(d, dirn))

    def wait(self, q, step, box, i):
        lanes = sum(self.lanes[k][1] * (1 if step > self.EARLY else self.lanes[k][2]) for k in self.classes(i))
        arrived(self.w.at[(*self.lead, *[pl.ds(0, m) for m in box], ALL, pl.ds(0, lanes))], self.sem(q, step, i))

    def end(self, step, i=0):
        self.wait(1, step, ((3, 1, 1), (3, 1, 1), (3, 3, 1), None, (1, R, R))[step], i)

    def drain(self):
        for step in (self.OWN, self.EARLY):
            self.wait(0, step, (3, 1, 1), 0)
        for i in range(max(n for _, _, n in self.lanes)):
            self.wait(0, self.RING, (3, 3, 1), i)
            self.wait(0, self.PLANE, (3, R, R), i)


PLAN = (
    ("end", 2, 11, 11107363011),
    ("second_end", 1, 9, 11013454310),
    ("middle", 1, 6, 11113162313),
    ("end", 0, 3, 12113122521),
    ("mid", 0, 1, 11211312133),
    ("start", 0, 0, 10112221212),
)
GIVE_SLOTS = (13, 15, 17, 18)
TAKE_SLOTS = (20, 22, 24, 26)
FIELD = 16


def slots_of(first, later):
    out = [first]
    for digit in str(later)[1:]:
        out.append(out[-1] + int(digit))
    return out


def how_many(slots, t):
    words = [sum(slots.count(FIELD * i + q) << (2 * q) for q in range(FIELD)) for i in range(LAST_SLOT // FIELD + 1)]
    word = jnp.int32(0)
    for i, value in enumerate(words):
        word = jnp.where(lax.div(t, FIELD) == i, jnp.int32(value - (value >> 31 << 32)), word)
    return lax.shift_right_logical(word, 2 * lax.rem(t, FIELD)) & 3


PLAN = [(name, ph, slots_of(*when)) for name, ph, *when in PLAN]
LAST_SLOT = max(q for *_, slots in PLAN for q in slots)


class Scatter:
    def __init__(self, pc, pool, recv, sems, credit, finish):
        self.pc, self.pool, self.recv, self.sems, self.credit, self.finish = pc, pool, recv, sems, credit, finish

    @staticmethod
    def place_of(u):
        v = u - U2
        return jnp.where(u < U2, 2 * U2 + u, R * lax.div(v, 2) + lax.rem(v, 2))

    def blk(self, u, k, ph, v, half):
        order = ORDERS[k]
        idx = [None] * len(order)
        for q in range(ph):
            idx[order[q]] = self.pc.c[order[q]]
        idx[order[ph]] = v
        free = [d for d in DIMS if idx[d] is None]
        for d in free:
            idx[d] = ALL
        if free:
            idx[free[0]] = part(half)
        return self.pool.at[(self.place_of(u), *idx)]

    def landing(self, n, k, ph, dirn, kind, half):
        r = self.recv[ph][kind]
        r = r.at[k, lax.rem(n, r.shape[1]), dirn]
        return r if half is None or not kind else r.at[part(half)]

    def ssem(self, n, pair, ph):
        return self.sems[0].at[(ph * 2 + pair) * SENDS + lax.rem(n, SENDS)]

    def rsem(self, n, pair, ph, kind):
        return self.sems[1].at[4 * sum(SLOTS[:ph]) + (pair * 2 + kind) * SLOTS[ph] + lax.rem(n, SLOTS[ph])]

    def send(self, n, k, ph, src, dst, kind, v):
        pair = k // 2
        remote(src, dst, self.ssem(n, pair, ph), self.rsem(n, pair, ph, kind), self.pc.dev(ORDERS[k][ph], v)).start()

    def copy(self, n, k, ph, dirn, kind):
        d = ORDERS[k][ph]
        near = self.pc.near(d, dirn)
        half = 1 - dirn if kind == 1 else dirn
        src = self.blk(n * 3 + k, k, ph, near if kind else self.pc.opp[d], half)
        dst = self.landing(n, k, ph, dirn, min(kind, 1), half)
        self.send(n, k, ph, src, dst, min(kind, 1), near)

    def start_short(self, n, ks):
        slot = lax.rem(n, SLOTS[1])
        for k in ks:
            slots = [self.recv[1][1].at[k, slot, i] for i in BOTH] + [self.recv[3][0].at[k]]
            for v, dst in zip(self.pc.others(ORDERS[k][1]), slots):
                self.send(n, k, 1, self.blk(n * 3 + k, k, 1, v, None), dst, 1, v)

    def end_short(self, n, ks):
        slot = lax.rem(n, SLOTS[1])
        arrived(self.recv[1][1].at[:, slot], self.rsem(n, 0, 1, 1))
        for k in ks:
            own = self.blk(n * 3 + k, k, 1, self.pc.c[ORDERS[k][1]], None)
            tot = own[...] + self.recv[3][0].at[k][...]
            for i in BOTH:
                tot = tot + self.recv[1][1].at[k, slot, i][...]
            own[...] = tot
        self.sent(n, 0, 1)
        self.start_last(n, ks)

    def received(self, n, pair, ph, kind):
        r, slot = self.recv[ph][kind], 0
        arrived(r.at[2, slot] if pair else r.at[pl.ds(0, 2), slot], self.rsem(n, pair, ph, kind))

    def sent(self, n, pair, ph):
        r = self.recv[ph][1]
        if ph < 2:
            ref = r.at[:, 0, 0] if pair else r.at[:, 0]
        else:
            ref = r.at[2, 0] if pair else r.at[pl.ds(0, 2), 0]
        arrived(ref, self.ssem(n, pair, ph))

    def start(self, n, ks, ph):
        if ph == 0:

            @pl.when(n >= FEW)
            def _():
                for k in ks:
                    for dirn in BOTH:
                        pl.semaphore_wait(self.credit.at[2 * k + dirn], 1)

        for kind in BOTH:
            for k in ks:
                for dirn in BOTH:
                    self.copy(n, k, ph, dirn, kind)

    def give_credit(self, ks):
        for k in ks:
            d = ORDERS[k][0]
            for dirn in BOTH:
                to = self.pc.dev(d, self.pc.near(d, dirn))
                pl.semaphore_signal(self.credit.at[2 * k + 1 - dirn], inc=1, device_id=to, device_id_type=MESH)

    def start_last(self, n, ks):
        for k in ks:
            for i, v in enumerate(self.pc.others(ORDERS[k][2])):
                self.send(n, k, 2, self.blk(n * 3 + k, k, 2, v, None), self.recv[2][1].at[k, lax.rem(n, SLOTS[2]), i], 1, v)

    @staticmethod
    def choose(n, ks, usual, short):
        if len(ks) == 1:
            usual()
        else:
            pl.when(n < SHORT)(usual)
            pl.when(n >= SHORT)(short)

    def middle(self, n, ks, ph):
        self.choose(n, ks, lambda: self.mid(n, ks, ph), lambda: None)

    def second_end(self, n, ks, ph):
        self.choose(n, ks, lambda: self.end(n, ks, ph), lambda: self.end_short(n, ks))

    def mid(self, n, ks, ph):
        self.received(n, ks[0] // 2, ph, 0)
        for k in ks:
            d = ORDERS[k][ph]
            for dirn in BOTH:
                b = self.blk(n * 3 + k, k, ph, self.pc.near(d, dirn), dirn)
                b[...] = b[...] + self.landing(n, k, ph, dirn, 0, None)[...]
        for k in ks:
            for dirn in BOTH:
                self.copy(n, k, ph, dirn, 2)
        if ph == 0:
            pl.when(n == 0)(lambda: self.give_credit(ks))

    def end(self, n, ks, ph):
        self.received(n, ks[0] // 2, ph, 1)
        for k in ks:
            own = self.blk(n * 3 + k, k, ph, self.pc.c[ORDERS[k][ph]], None)
            tot = own[...]
            for i in range(3 if ph == 2 else 2):
                tot = tot + self.recv[ph][1].at[k, lax.rem(n, SLOTS[ph]), i][...]
            if ph < 2:
                own[...] = tot
            else:
                self.finish(n * 3 + k, tot)
        self.sent(n, ks[0] // 2, ph)
        if ph == 0:
            self.choose(n, ks, lambda: self.start(n, ks, 1), lambda: self.start_short(n, ks))

            pl.when(n + SLOTS[0] < ROUNDS[ks[0]])(lambda: self.give_credit(ks))
        elif ph == 1:
            self.start_last(n, ks)

    def events(self, t, come):
        out = []
        for (name, ph, slots), first in zip(PLAN, come):

            def step(n, _):
                for ks in PAIRS:
                    take = lambda: getattr(self, name)(n, ks, ph)
                    pl.when(n < ROUNDS[ks[0]])(take) if ROUNDS[ks[0]] < max(ROUNDS) else take()
                return 0

            out.append(first + how_many(slots, t))
            lax.fori_loop(first, out[-1], step, 0)
        return tuple(out)


def half_tanh(h, h2):
    return 0.5 * jnp.tanh(h * (C0 + C1 * h2))


def gelu(h):
    return h * (0.5 + half_tanh(h, h * h))


def gelu_slope(h):
    h2 = h * h
    t = half_tanh(h, h2)
    return (0.5 + t) + ((0.25 - t * t) * (2.0 * C0 + (6.0 * C1) * h2)) * h


def recv_shapes():
    out = []
    for ph, dims in enumerate(((R, R), (R,))):
        for q in ((2, *dims[1:]), dims):
            out.append((3, SLOTS[ph] if ph or q == dims else FEW, 2, *q, SUBL, COL))
    return out + [(3, SLOTS[2], 3, SUBL, COL), (2, R, SUBL, COL)]


AG1, AG2 = Gather.count(W1_LANES), Gather.count(W2_LANES)
BLOCKS = DIM // COL


def kernel(xh, uph, dnh, gh, y, gx, dw1o, dw2o, landh, keeph, xp, xt, gp, w1, w2, a, pool, sb, dw1s, *rest):
    recv, (ag_s, ag_r, rs_s, rs_r, lsem, xs, xr, spare_sem, credit) = rest[:6], rest[6:]
    pc = Place()
    s = pc.s
    my_lanes, their_lanes = span(s, HALF), span(1 - s, HALF)
    scope = jax.named_scope
    tokens_x, tokens_g = (y, xp), (gx, gp)

    loads = [
        pltpu.make_async_copy(src, dst, lsem.at[i])
        for i, (src, dst) in enumerate((
            (uph.at[:, my_lanes], w1.at[(s, *pc.c)]),
            (dnh, w2.at[tuple(pc.c)]),
            (xh, y),
            (gh, gx),
        ))
    ]
    for c in loads:
        c.start()

    with scope("bar"):
        bar = pltpu.get_barrier_semaphore()
        peers = [pc.partner] + [pc.dev(d, v) for d in DIMS for v in pc.others(d)]
        for dev in peers:
            pl.semaphore_signal(bar, inc=1, device_id=dev, device_id_type=MESH)
        pl.semaphore_wait(bar, len(peers))

    swaps = [
        remote(src, dst, xs.at[i], xr.at[i], pc.partner)
        for i, (src, dst) in enumerate((
            (uph.at[:, their_lanes], w1.at[(s, *pc.c)]),
            (xh, xp),
            (gh, gp),
        ))
    ]
    for c in swaps:
        c.start()

    g1 = Gather(pc, w1, (ALL,), W1_LANES, (ag_s, ag_r), 0)
    g2 = Gather(pc, w2, (), W2_LANES, (ag_s, ag_r), AG1)

    w1f = w1.reshape(DIM, HALF)
    w2f = w2.reshape(HALF, DIM)
    units = pool.reshape(3 * U2, R * R * R, SUBL, COL)

    with scope("swapw"):
        loads[0].wait()
        swaps[0].wait_recv()
    own, early, ring, plane, halves = range(5)
    g1.start(own)
    loads[1].wait()
    g2.start(own)
    g1.start(early)
    g2.start(early)
    with scope("own"):
        g1.end(own)
    for i in range(3):
        g1.start(ring, i)
    with scope("owntwo"):
        g2.end(own)
    for i in range(3):
        g2.start(ring, i)
    with scope("early"):
        g1.end(early)
    for i in BOTH:
        with scope("ring"):
            g1.end(ring, i)
        g1.start(plane, i)
    with scope("mid"):
        g1.mid(0)
    with scope("ring"):
        g1.end(ring, 2)
    g1.start(plane, 2)
    with scope("mid"):
        g1.mid(1)
    with scope("ringtwo"):
        g2.end(early)
        g2.end(ring, 0)
    g2.start(plane, 0)
    def turn(i, _):
        for q, part_x in enumerate(tokens_x):
            xt[:, pl.ds(pl.multiple_of(q * TOK + i * COL, COL), COL)] = part_x[span(i, COL), :].T
        return 0

    loads[2].wait()
    swaps[1].wait_recv()
    with scope("turn"):
        lax.fori_loop(0, TOK // COL, turn, 0)

    def rows(i):
        return slice(STEP * i, STEP * (i + 1))

    def step_of(pair, i):
        return pair[i // 2][rows(i % 2), :]

    def flat(c, i):
        return units.at[R * c + i]

    def hidden_dot(c, i):
        sb[i % 2, :STEP] = dot(step_of(tokens_x, i), w1f[:, span(c, COL)], NN)

    def hidden_act(c, i):
        h = sb[i % 2, :STEP]
        flat(c, i)[...] = h.reshape(STEP // SUBL, SUBL, COL)
        a[rows(i), span(c, COL)] = gelu(h).astype(bf16)

    def dhidden_dot(c, i):
        sb[i] = dot(tokens_g[i][...], w2f[span(c, COL), :], NT)

    def dhidden_act(c, i):
        for h in BOTH:
            slope = gelu_slope(flat(c, 2 * i + h)[...].reshape(STEP, COL))
            a[rows(2 * i + h), span(c, COL)] = (slope * sb[i, rows(h)]).astype(bf16)

    def grad1(c):
        r = dot(xt[...], a[:, span(c, COL)], NN)
        for p in BOTH:
            flat(c, p)[...] = r[rows(p)].reshape(STEP // SUBL, SUBL, COL)

    def chunk_steps(steps, dot_step, act_step, c, after):
        for i in range(steps):
            if i + 1 < steps:
                dot_step(c, i + 1)
            else:
                dot_step(after, 0)
            act_step(c, i)

    def grad2_rows(c, nb):
        cols = pl.ds(nb * 2 * COL, 2 * COL)
        both = jnp.concatenate([q[:, cols] for q in tokens_g])
        r = dot(a[:, span(c, COL)], both, TN)
        for b in BOTH:
            rr = r[:, COL * b:COL * (b + 1)].reshape(SUBL, R, SUBL, COL)
            for q in range(R):
                units[2 * U2 + R * (2 * nb + b) + q, span(c, SUBL)] = rr[:, q]

    def grad2_half(i, nb):
        for q in range(R):
            grad2_rows(i * R + q, nb)

    own, theirs = pl.ds(0, TOK), pl.ds(TOK, TOK)

    def product(at, nb, i):
        lanes = span(nb, COL)
        return dot(a[at, :], w1f[lanes, :], NT) if i else dot(a[at, :], w2f[:, lanes], NN)

    def keep_y(n):
        return pltpu.make_async_copy(sb.at[lax.rem(n, 3)], keeph.at[n], lsem.at[R + lax.rem(n, 3)])

    def give_y_block(nb):
        return remote(keeph.at[2 * nb], landh.at[nb], xs.at[3 + nb], xr.at[3 + nb], pc.partner)

    def kept(n):
        keep_y(n).wait()

        @pl.when(lax.rem(n, 2) == 0)
        def _():
            give_y_block(lax.div(n, 2)).start()

    def give_y(n):
        @pl.when(n > 2)
        def _():
            kept(n - 3)

        at = span(1 - lax.rem(n, 2), TOK)
        sb[lax.rem(n, 3)] = product(at, lax.div(n, 2), 0)
        keep_y(n).start()

    def finish_block(nb, res, at, part_sum):
        lanes = span(nb, COL)
        res[at, lanes] = (res[at, lanes].astype(f32) + part_sum).astype(bf16)

    def fetched_y(nb):
        return [pltpu.make_async_copy(src, sb.at[b], lsem.at[R + b]) for b, src in enumerate((landh.at[nb], keeph.at[2 * nb + 1]))]

    def fetch_y(nb):
        give_y_block(nb).wait_recv()
        for c in fetched_y(nb):
            c.start()

    def take_y(nb):
        for c in fetched_y(nb):
            c.wait()

        def add(h, _):
            finish_block(nb, y, span(h, COL), sb[0, span(h, COL)] + sb[1, span(h, COL)])
            return 0

        lax.fori_loop(0, TOK // COL, add, 0)

    def spare(n):
        return units.at[pl.ds(R * n + 2, 2)]

    def give_gx_block(nb):
        return remote(spare(BLOCKS + nb), spare(nb), xs.at[3 + BLOCKS + nb], xr.at[3 + BLOCKS + nb], pc.partner)

    def give_gx(nb):
        spare(BLOCKS + nb)[...] = product(theirs, nb, 1).reshape(2, TOK // 2 // SUBL, SUBL, COL)
        give_gx_block(nb).start()

    def take_gx(nb):
        give_gx_block(nb).wait_recv()

        def add(h, _):
            at = span(h, STEP)
            finish_block(nb, gx, at, product(at, nb, 1) + flat(nb, 2 + h)[...].reshape(STEP, COL))
            return 0

        lax.fori_loop(0, TOK // STEP, add, 0)

    def loop(n, fn):
        def body(i, _):
            fn(i)
            return 0

        lax.fori_loop(0, n, body, 0)

    def at(t, first, fn, last=None):
        @pl.when((t >= first) & (t <= (first if last is None else last)))
        def _():
            with scope(f"task{first}"):
                fn()

    def last_sends():
        g1.mid(2)
        for i in (1, 2):
            g2.end(ring, i)
            g2.start(plane, i)

    def columns(i, _):
        n = jnp.where(i < 2, 3, 2)

        def step(q, _):
            at(3 * i + q, 1, last_sends)
            for sub, when in enumerate((3, 6, 6)):
                at(3 * i + q, when, lambda: g2.mid(sub))
            last = q == n - 1
            for nxt in (1, 2):

                @pl.when(last & (i + 1 == nxt))
                def _():
                    with scope("arrive"):
                        g1.end(halves, nxt)

            after = jnp.where(last, jnp.minimum(i + 1, CHUNKS - 6), i + 3 * q + 3)
            chunk_steps(STEPS, hidden_dot, hidden_act, i + 3 * q, after)
            return 0

        with scope("hidden"):
            lax.fori_loop(0, n, step, 0)
        with scope("gradtwo"):
            for last in (1, 2):

                @pl.when((i < 2) if last == 2 else (i == 2))
                def _():
                    for q in range(last + 1):
                        grad2_rows(i + 3 * q, 0)

        return 0

    with scope("arrive"):
        g1.end(halves, 0)
    hidden_dot(0, 0)
    loads[3].wait()
    swaps[2].wait_recv()
    lax.fori_loop(0, 3, columns, 0)

    def finish(u, tot):
        @pl.when(u < U2)
        def _():
            dw2o[span(lax.rem(u, R), SUBL), span(lax.div(u, R), COL)] = tot

        @pl.when(u >= U2)
        def _():
            v = u - U2
            q = lax.div(v, 2)

            @pl.when(lax.rem(v, 2) == s)
            def _():
                dw1o[:, pl.ds(pl.multiple_of(HALF * s + COL * q, COL), COL)] = tot

            @pl.when(lax.rem(v, 2) != s)
            def _():
                dw1s[:, span(q, COL)] = tot

    rs = Scatter(pc, pool, [recv[:2], recv[2:4], (None, recv[4]), recv[5:]], (rs_s, rs_r), credit, finish)

    def first_dot():
        for n in range(3):
            kept(2 * BLOCKS - 3 + n)
        dhidden_dot(0, 0)

    def dhidden(c):
        chunk_steps(2, dhidden_dot, dhidden_act, c, jnp.minimum(c + 1, CHUNKS - 1))
        grad1(c)

    def settle():
        for i in range(3):
            g2.end(halves, i)
        g1.drain()
        g2.drain()

    def slot(t, come):
        with scope("ev"):
            come = (*rs.events(t, come[:-2]), *come[-2:])

        at(t, 0, lambda: loop(2, lambda i: grad2_half(i, 1)))
        at(t, 1, settle)
        at(t, 1, lambda: loop(2, lambda i: give_y(2 * (t - 1) + i)), 4)
        at(t, 5, first_dot)
        at(t, 5, lambda: dhidden(t - 5), 12)
        at(t, 9, lambda: pl.semaphore_signal(spare_sem, inc=1, device_id=pc.partner, device_id_type=MESH))
        at(t, GIVE_SLOTS[0], lambda: pl.semaphore_wait(spare_sem, 1))

        def tokens(nb):
            fetch_y(nb)
            give_gx(nb)
            take_y(nb)

        *come, given, taken = come
        for slots, task, done in ((GIVE_SLOTS, tokens, given), (TAKE_SLOTS, take_gx, taken)):
            come.append(done + how_many(slots, t))
            pl.when(come[-1] > done)(lambda: task(done))
        return tuple(come)

    lax.fori_loop(0, LAST_SLOT + 1, slot, (jnp.int32(0),) * (len(PLAN) + 2))

    with scope("last"):
        last = remote(dw1s, dw1o.at[:, my_lanes], xs.at[11], xr.at[11], pc.partner)
        last.start()
        for c in swaps:
            c.wait_send()
        for nb in range(BLOCKS):
            give_y_block(nb).wait_send()
            give_gx_block(nb).wait_send()
        last.wait()


def copy_out(*refs):
    n = len(refs) // 2
    copies = [pltpu.make_async_copy(src, dst, refs[-1].at[i]) for i, (src, dst) in enumerate(zip(refs[:n], refs[n:]))]
    for c in copies:
        c.start()
    for c in copies:
        c.wait()


def local_stack(x, up, down, g):
    shape = jax.ShapeDtypeStruct
    dma = pltpu.SemaphoreType.DMA
    bf = [(TOK, DIM), (DIM, 2 * TOK), (TOK, DIM), (2, R, R, R, SUBL, HALF), (R, R, R, HALF // R**3, DIM), (2 * TOK, HALF)]
    ff = [(3 * U2, R, R, R, SUBL, COL), (3, TOK, COL), (SUBL, HALF)] + recv_shapes()
    results = [(x.shape, bf16), (g.shape, bf16), (up.shape[1:], f32), (down.shape[1:], f32)]
    res = pl.pallas_call(
        kernel,
        out_shape=[pltpu.VMEM(*q) for q in results] + [shape((n, TOK, COL), f32) for n in (BLOCKS, 2 * BLOCKS)],
        in_specs=[ANY] * 4,
        out_specs=[VMEM] * 4 + [ANY] * 2,
        scratch_shapes=[pltpu.VMEM(q, bf16) for q in bf] + [pltpu.VMEM(q, f32) for q in ff]
        + [dma((n,)) for n in (AG1 + AG2, AG1 + AG2, 6 * SENDS, 4 * sum(SLOTS), 7, 12, 12)]
        + [pltpu.SemaphoreType.REGULAR, pltpu.SemaphoreType.REGULAR((6,))],
        compiler_params=pltpu.CompilerParams(collective_id=0, has_side_effects=True, vmem_limit_bytes=62586880),
        name="stack",
    )(x, up[0], down[0], g)[:4]
    y, gx, dw1, dw2 = pl.pallas_call(
        copy_out,
        out_shape=[shape(*q) for q in results],
        in_specs=[VMEM] * 4,
        out_specs=[ANY] * 4,
        scratch_shapes=[dma((4,))],
        compiler_params=pltpu.CompilerParams(vmem_limit_bytes=2**23),
        name="copy_out",
    )(*res)
    return y, gx, dw1[None], dw2[None]


def solution(mesh):
    tok, mat = P(AXES, None), P(None, AXES, None)
    return jax.shard_map(local_stack, mesh=mesh, in_specs=(tok, mat, mat, tok), out_specs=(tok, tok, mat, mat), check_vma=False)
```

```python
import jax
import jax.numpy as jnp
from jax import lax
from jax.experimental import pallas as pl
from jax.experimental.pallas import tpu as pltpu
from jax.sharding import PartitionSpec as P

f32, bf16 = jnp.float32, jnp.bfloat16
MESH = pl.DeviceIdType.MESH
NN, NT, TN = [(((i,), (k,)), ((), ())) for i, k in ((1, 0), (1, 1), (0, 0))]
ANY = pl.BlockSpec(memory_space=pl.ANY)
VMEM = pl.BlockSpec(memory_space=pltpu.VMEM)
AXES = ("sub", "fsdp")

TOK = 1024
DIM = 1024
HALF = 2048
R = 4
SUBL, LANES = 8, 128
COL = 256
CHUNKS = HALF // COL
STEP = 512
STEPS = 2 * TOK // STEP
DH_BUFFERS = (2, 0)
Y_SLOT, DH_SLOT = 4, 8
U2 = 16
SLOTS = (4, 5, 5)
FEW = 3
SENDS = 4
ROUNDS = (11, 11, 10)
SHORT = 10
CLASSES = DIMS = range(3)
PAIRS = ((0, 1), (2,))
BOTH = range(2)
ORDERS = ((0, 1, 2), (1, 2, 0), (2, 0, 1))
STRIDE = (R * R, R, 1)
C0 = 0.7978845608028654
C1 = 0.044715 * C0
ALL = slice(None)

W1_LANES = ((0, COL, 3), (3 * COL, COL, 3), (6 * COL, COL, 2))
W2_LANES = ((0, LANES, 2), (2 * LANES, LANES, 3), (5 * LANES, LANES, 3))


def dot(a, b, dims):
    return lax.dot_general(a, b, dims, preferred_element_type=f32)


def span(i, n):
    return pl.ds(pl.multiple_of(i * n, n), n)


class Place:
    def __init__(self):
        self.s, self.j = lax.axis_index("sub"), lax.axis_index("fsdp")
        self.c = [lax.rem(lax.div(self.j, n), R) for n in STRIDE]
        self.plus, self.minus, self.opp = [[lax.rem(c + o, R) for c in self.c] for o in (1, 3, 2)]
        self.partner = (1 - self.s, self.j)

    def dev(self, d, v):
        return (self.s, self.j + (v - self.c[d]) * STRIDE[d])

    def near(self, d, dirn):
        return self.minus[d] if dirn else self.plus[d]

    def others(self, d):
        return self.plus[d], self.minus[d], self.opp[d]


def remote(src, dst, ssem, rsem, dev):
    return pltpu.make_async_remote_copy(src, dst, ssem, rsem, device_id=dev, device_id_type=MESH)


def arrived(ref, sem):
    pltpu.make_async_copy(ref, ref, sem).wait()


def part(half):
    return ALL if half is None else pl.ds(2 * half, 2)


class Gather:
    OWN, EARLY, RING, PLANE, HALVES = range(5)

    def __init__(self, pc, w, lead, lanes, sems, base):
        self.pc, self.w, self.lead, self.lanes, self.sems, self.base = pc, w, lead, lanes, sems, base

    @staticmethod
    def count(lanes):
        return 2 + 3 * max(n for _, _, n in lanes)

    def at(self, ln, changes):
        idx = list(self.pc.c)
        for d, v in changes:
            idx[d] = v
        return self.w.at[(*self.lead, *idx, ALL, ln)]

    def classes(self, i):
        return [k for k in CLASSES if i < self.lanes[k][2]]

    def stretch(self, k, step, i):
        lane0, width, subs = self.lanes[k]
        return pl.ds(lane0, width * subs) if step < self.RING else pl.ds(lane0 + i * width, width)

    def sem(self, q, step, i):
        return self.sems[q].at[self.base + step + 3 * i]

    def send(self, block, step, into, i, d, v):
        remote(block, block, self.sem(0, step, i), self.sem(1, into, i), self.pc.dev(d, v)).start()

    def start(self, step, i=0):
        for k in self.classes(i):
            ln = self.stretch(k, step, i)
            d1, d2, d3 = ORDERS[k]
            d = (d1, d2, d2, d3)[step]
            if step < self.RING:
                blocks = [self.at(ln, ())]
            elif step == self.RING:
                blocks = [self.at(ln, ((d1, v),)) for v in self.pc.others(d1)]
            else:
                blocks = [self.at(ln, ((d1, ALL), (d2, ALL)))]
            for v in self.pc.others(d)[:3 if step < self.PLANE else 2]:
                for block in blocks:
                    self.send(block, step, step, i, d, v)

    def mid(self, i=0):
        self.wait(1, self.PLANE, (2, R, R), i)
        for k in self.classes(i):
            d1, d2, d = ORDERS[k]
            for dirn in BOTH:
                behind = self.pc.near(d, 1 - dirn)
                block = self.at(self.stretch(k, self.PLANE, i), ((d1, part(dirn)), (d2, ALL), (d, behind)))
                self.send(block, self.PLANE, self.HALVES, i, d, self.pc.near(d, dirn))

    def wait(self, q, step, box, i):
        lanes = sum(self.lanes[k][1] * (1 if step > self.EARLY else self.lanes[k][2]) for k in self.classes(i))
        arrived(self.w.at[(*self.lead, *[pl.ds(0, m) for m in box], ALL, pl.ds(0, lanes))], self.sem(q, step, i))

    def end(self, step, i=0):
        self.wait(1, step, ((3, 1, 1), (3, 1, 1), (3, 3, 1), None, (1, R, R))[step], i)

    def drain(self):
        for step in (self.OWN, self.EARLY):
            self.wait(0, step, (3, 1, 1), 0)
        for i in range(max(n for _, _, n in self.lanes)):
            self.wait(0, self.RING, (3, 3, 1), i)
            self.wait(0, self.PLANE, (3, R, R), i)


PLAN = (
    ("end", 2, 13, 13233233111),
    ("second_end", 1, 11, 11232252201),
    ("middle", 1, 9, 11221244202),
    ("end", 0, 6, 12203213421),
    ("mid", 0, 4, 11211312313),
    ("start", 0, 2, 11112221221),
)
GIVE_SLOTS = (16, 18, 20, 21)
TAKE_SLOTS = (22, 23, 25, 27)
FIELD = 16


def slots_of(first, later):
    out = [first]
    for digit in str(later)[1:]:
        out.append(out[-1] + int(digit))
    return out


def how_many(slots, t):
    words = [sum(slots.count(FIELD * i + q) << (2 * q) for q in range(FIELD)) for i in range(LAST_SLOT // FIELD + 1)]
    word = jnp.int32(0)
    for i, value in enumerate(words):
        word = jnp.where(lax.div(t, FIELD) == i, jnp.int32(value - (value >> 31 << 32)), word)
    return lax.shift_right_logical(word, 2 * lax.rem(t, FIELD)) & 3


PLAN = [(name, ph, slots_of(*when)) for name, ph, *when in PLAN]
LAST_SLOT = max(q for *_, slots in PLAN for q in slots)


class Scatter:
    def __init__(self, pc, pool, recv, sems, credit, finish):
        self.pc, self.pool, self.recv, self.sems, self.credit, self.finish = pc, pool, recv, sems, credit, finish

    @staticmethod
    def place_of(u):
        v = u - U2
        return jnp.where(u < U2, 2 * U2 + u, R * lax.div(v, 2) + lax.rem(v, 2))

    def blk(self, u, k, ph, v, half):
        order = ORDERS[k]
        idx = [None] * len(order)
        for q in range(ph):
            idx[order[q]] = self.pc.c[order[q]]
        idx[order[ph]] = v
        free = [d for d in DIMS if idx[d] is None]
        for d in free:
            idx[d] = ALL
        if free:
            idx[free[0]] = part(half)
        return self.pool.at[(self.place_of(u), *idx)]

    def landing(self, n, k, ph, dirn, kind, half):
        r = self.recv[ph][kind]
        r = r.at[k, lax.rem(n, r.shape[1]), dirn]
        return r if half is None or not kind else r.at[part(half)]

    def ssem(self, n, pair, ph):
        return self.sems[0].at[(ph * 2 + pair) * SENDS + lax.rem(n, SENDS)]

    def rsem(self, n, pair, ph, kind):
        return self.sems[1].at[4 * sum(SLOTS[:ph]) + (pair * 2 + kind) * SLOTS[ph] + lax.rem(n, SLOTS[ph])]

    def send(self, n, k, ph, src, dst, kind, v):
        pair = k // 2
        remote(src, dst, self.ssem(n, pair, ph), self.rsem(n, pair, ph, kind), self.pc.dev(ORDERS[k][ph], v)).start()

    def copy(self, n, k, ph, dirn, kind):
        d = ORDERS[k][ph]
        near = self.pc.near(d, dirn)
        half = 1 - dirn if kind == 1 else dirn
        src = self.blk(n * 3 + k, k, ph, near if kind else self.pc.opp[d], half)
        dst = self.landing(n, k, ph, dirn, min(kind, 1), half)
        self.send(n, k, ph, src, dst, min(kind, 1), near)

    def start_short(self, n, ks):
        slot = lax.rem(n, SLOTS[1])
        for k in ks:
            slots = [self.recv[1][1].at[k, slot, i] for i in BOTH] + [self.recv[3][0].at[k]]
            for v, dst in zip(self.pc.others(ORDERS[k][1]), slots):
                self.send(n, k, 1, self.blk(n * 3 + k, k, 1, v, None), dst, 1, v)

    def end_short(self, n, ks):
        slot = lax.rem(n, SLOTS[1])
        arrived(self.recv[1][1].at[:, slot], self.rsem(n, 0, 1, 1))
        for k in ks:
            own = self.blk(n * 3 + k, k, 1, self.pc.c[ORDERS[k][1]], None)
            tot = own[...] + self.recv[3][0].at[k][...]
            for i in BOTH:
                tot = tot + self.recv[1][1].at[k, slot, i][...]
            own[...] = tot
        self.sent(n, 0, 1)
        self.start_last(n, ks)

    def received(self, n, pair, ph, kind):
        r, slot = self.recv[ph][kind], 0
        arrived(r.at[2, slot] if pair else r.at[pl.ds(0, 2), slot], self.rsem(n, pair, ph, kind))

    def sent(self, n, pair, ph):
        r = self.recv[ph][1]
        if ph < 2:
            ref = r.at[:, 0, 0] if pair else r.at[:, 0]
        else:
            ref = r.at[2, 0] if pair else r.at[pl.ds(0, 2), 0]
        arrived(ref, self.ssem(n, pair, ph))

    def start(self, n, ks, ph):
        if ph == 0:

            @pl.when(n >= FEW)
            def _():
                for k in ks:
                    for dirn in BOTH:
                        pl.semaphore_wait(self.credit.at[2 * k + dirn], 1)

        for kind in BOTH:
            for k in ks:
                for dirn in BOTH:
                    self.copy(n, k, ph, dirn, kind)

    def give_credit(self, ks):
        for k in ks:
            d = ORDERS[k][0]
            for dirn in BOTH:
                to = self.pc.dev(d, self.pc.near(d, dirn))
                pl.semaphore_signal(self.credit.at[2 * k + 1 - dirn], inc=1, device_id=to, device_id_type=MESH)

    def start_last(self, n, ks):
        for k in ks:
            for i, v in enumerate(self.pc.others(ORDERS[k][2])):
                self.send(n, k, 2, self.blk(n * 3 + k, k, 2, v, None), self.recv[2][1].at[k, lax.rem(n, SLOTS[2]), i], 1, v)

    @staticmethod
    def choose(n, ks, usual, short):
        if len(ks) == 1:
            usual()
        else:
            pl.when(n < SHORT)(usual)
            pl.when(n >= SHORT)(short)

    def middle(self, n, ks, ph):
        self.choose(n, ks, lambda: self.mid(n, ks, ph), lambda: None)

    def second_end(self, n, ks, ph):
        self.choose(n, ks, lambda: self.end(n, ks, ph), lambda: self.end_short(n, ks))

    def mid(self, n, ks, ph):
        self.received(n, ks[0] // 2, ph, 0)
        for k in ks:
            d = ORDERS[k][ph]
            for dirn in BOTH:
                b = self.blk(n * 3 + k, k, ph, self.pc.near(d, dirn), dirn)
                b[...] = b[...] + self.landing(n, k, ph, dirn, 0, None)[...]
        for k in ks:
            for dirn in BOTH:
                self.copy(n, k, ph, dirn, 2)
        if ph == 0:
            pl.when(n == 0)(lambda: self.give_credit(ks))

    def end(self, n, ks, ph):
        self.received(n, ks[0] // 2, ph, 1)
        for k in ks:
            own = self.blk(n * 3 + k, k, ph, self.pc.c[ORDERS[k][ph]], None)
            tot = own[...]
            for i in range(3 if ph == 2 else 2):
                tot = tot + self.recv[ph][1].at[k, lax.rem(n, SLOTS[ph]), i][...]
            if ph < 2:
                own[...] = tot
            else:
                self.finish(n * 3 + k, tot)
        self.sent(n, ks[0] // 2, ph)
        if ph == 0:
            self.choose(n, ks, lambda: self.start(n, ks, 1), lambda: self.start_short(n, ks))

            pl.when(n + SLOTS[0] < ROUNDS[ks[0]])(lambda: self.give_credit(ks))
        elif ph == 1:
            self.start_last(n, ks)

    def events(self, t, come):
        out = []
        for (name, ph, slots), first in zip(PLAN, come):

            def step(n, _):
                for ks in PAIRS:
                    take = lambda: getattr(self, name)(n, ks, ph)
                    pl.when(n < ROUNDS[ks[0]])(take) if ROUNDS[ks[0]] < max(ROUNDS) else take()
                return 0

            out.append(first + how_many(slots, t))
            lax.fori_loop(first, out[-1], step, 0)
        return tuple(out)


def half_tanh(h, h2):
    return 0.5 * jnp.tanh(h * (C0 + C1 * h2))


def gelu(h):
    return h * (0.5 + half_tanh(h, h * h))


def gelu_slope(h):
    h2 = h * h
    t = half_tanh(h, h2)
    return (0.5 + t) + ((0.25 - t * t) * (2.0 * C0 + (6.0 * C1) * h2)) * h


def recv_shapes():
    out = []
    for ph, dims in enumerate(((R, R), (R,))):
        for q in ((2, *dims[1:]), dims):
            out.append((3, SLOTS[ph] if ph or q == dims else FEW, 2, *q, SUBL, COL))
    return out + [(3, SLOTS[2], 3, SUBL, COL), (2, R, SUBL, COL)]


AG1, AG2 = Gather.count(W1_LANES), Gather.count(W2_LANES)
BLOCKS = DIM // COL


def kernel(xh, uph, dnh, gh, y, gx, dw1o, dw2o, landh, keeph, xp, xt, gp, w1, w2, a, pool, sb, dw1s, *rest):
    recv, (ag_s, ag_r, rs_s, rs_r, lsem, xs, xr, spare_sem, credit) = rest[:6], rest[6:]
    pc = Place()
    s = pc.s
    my_lanes, their_lanes = span(s, HALF), span(1 - s, HALF)
    scope = jax.named_scope
    tokens_x, tokens_g = (y, xp), (gx, gp)

    loads = [
        pltpu.make_async_copy(src, dst, lsem.at[i])
        for i, (src, dst) in enumerate((
            (uph.at[:, my_lanes], w1.at[(s, *pc.c)]),
            (dnh, w2.at[tuple(pc.c)]),
            (xh, y),
            (gh, gx),
        ))
    ]
    for c in loads:
        c.start()

    with scope("bar"):
        bar = pltpu.get_barrier_semaphore()
        peers = [pc.partner] + [pc.dev(d, v) for d in DIMS for v in pc.others(d)]
        for dev in peers:
            pl.semaphore_signal(bar, inc=1, device_id=dev, device_id_type=MESH)
        pl.semaphore_wait(bar, len(peers))

    swaps = [
        remote(src, dst, xs.at[i], xr.at[i], pc.partner)
        for i, (src, dst) in enumerate((
            (uph.at[:, their_lanes], w1.at[(s, *pc.c)]),
            (xh, xp),
            (gh, gp),
        ))
    ]
    for c in swaps:
        c.start()

    g1 = Gather(pc, w1, (ALL,), W1_LANES, (ag_s, ag_r), 0)
    g2 = Gather(pc, w2, (), W2_LANES, (ag_s, ag_r), AG1)

    w1f = w1.reshape(DIM, HALF)
    w2f = w2.reshape(HALF, DIM)
    units = pool.reshape(3 * U2, R * R * R, SUBL, COL)

    with scope("swapw"):
        loads[0].wait()
        swaps[0].wait_recv()
    own, early, ring, plane, halves = range(5)
    g1.start(own)
    loads[1].wait()
    g2.start(own)
    g1.start(early)
    g2.start(early)
    with scope("own"):
        g1.end(own)
    for i in range(3):
        g1.start(ring, i)
    with scope("owntwo"):
        g2.end(own)
    for i in range(3):
        g2.start(ring, i)
    with scope("early"):
        g1.end(early)
    for i in BOTH:
        with scope("ring"):
            g1.end(ring, i)
        g1.start(plane, i)
    with scope("mid"):
        g1.mid(0)
    with scope("ring"):
        g1.end(ring, 2)
    g1.start(plane, 2)
    with scope("mid"):
        g1.mid(1)
    with scope("ringtwo"):
        g2.end(early)
        g2.end(ring, 0)
    g2.start(plane, 0)
    def turn(i, _):
        for q, part_x in enumerate(tokens_x):
            xt[:, pl.ds(pl.multiple_of(q * TOK + i * COL, COL), COL)] = part_x[span(i, COL), :].T
        return 0

    loads[2].wait()
    swaps[1].wait_recv()
    with scope("turn"):
        lax.fori_loop(0, TOK // COL, turn, 0)

    def rows(i):
        return slice(STEP * i, STEP * (i + 1))

    def step_of(pair, i):
        return pair[i // 2][rows(i % 2), :]

    def flat(c, i):
        return units.at[R * c + i]

    def hidden_dot(c, i):
        sb[i % 2, :STEP] = dot(step_of(tokens_x, i), w1f[:, span(c, COL)], NN)

    def hidden_act(c, i):
        h = sb[i % 2, :STEP]
        flat(c, i)[...] = h.reshape(STEP // SUBL, SUBL, COL)
        a[rows(i), span(c, COL)] = gelu(h).astype(bf16)

    def dhidden_dot(c, i):
        sb[DH_BUFFERS[i]] = dot(tokens_g[i][...], w2f[span(c, COL), :], NT)

    def dhidden_act(c, i):
        for h in BOTH:
            slope = gelu_slope(flat(c, 2 * i + h)[...].reshape(STEP, COL))
            a[rows(2 * i + h), span(c, COL)] = (slope * sb[DH_BUFFERS[i], rows(h)]).astype(bf16)

    def grad1(c):
        r = dot(xt[...], a[:, span(c, COL)], NN)
        for p in BOTH:
            flat(c, p)[...] = r[rows(p)].reshape(STEP // SUBL, SUBL, COL)

    def chunk_steps(steps, dot_step, act_step, c, after):
        for i in range(steps):
            if i + 1 < steps:
                dot_step(c, i + 1)
            else:
                dot_step(after, 0)
            act_step(c, i)

    def grad2(b):
        both = jnp.concatenate([q[:, span(b, COL)] for q in tokens_g])
        for c in range(CHUNKS):
            r = dot(a[:, COL * c:COL * (c + 1)], both, TN).reshape(SUBL, R, SUBL, COL)
            for q in range(R):
                units[2 * U2 + R * b + q, SUBL * c:SUBL * (c + 1)] = r[:, q]

    own, theirs = pl.ds(0, TOK), pl.ds(TOK, TOK)

    def product(at, nb, i):
        lanes = span(nb, COL)
        return dot(a[at, :], w1f[lanes, :], NT) if i else dot(a[at, :], w2f[:, lanes], NN)

    def keep_y(n):
        return pltpu.make_async_copy(sb.at[lax.rem(n, 3)], keeph.at[n], lsem.at[R + lax.rem(n, 3)])

    def give_y_block(nb):
        return remote(keeph.at[2 * nb], landh.at[nb], xs.at[3 + nb], xr.at[3 + nb], pc.partner)

    def kept(n):
        keep_y(n).wait()

        @pl.when(lax.rem(n, 2) == 0)
        def _():
            give_y_block(lax.div(n, 2)).start()

    def give_y(n):
        @pl.when(n > 2)
        def _():
            kept(n - 3)

        at = span(1 - lax.rem(n, 2), TOK)
        sb[lax.rem(n, 3)] = product(at, lax.div(n, 2), 0)
        keep_y(n).start()

    def finish_block(nb, res, at, part_sum):
        lanes = span(nb, COL)
        res[at, lanes] = (res[at, lanes].astype(f32) + part_sum).astype(bf16)

    def fetched_y(nb):
        return [pltpu.make_async_copy(src, sb.at[b], lsem.at[R + b]) for b, src in enumerate((landh.at[nb], keeph.at[2 * nb + 1]))]

    def fetch_y(nb):
        give_y_block(nb).wait_recv()
        for c in fetched_y(nb):
            c.start()

    def take_y(nb):
        for c in fetched_y(nb):
            c.wait()

        def add(h, _):
            finish_block(nb, y, span(h, COL), sb[0, span(h, COL)] + sb[1, span(h, COL)])
            return 0

        lax.fori_loop(0, TOK // COL, add, 0)

    def spare(n):
        return units.at[pl.ds(R * n + 2, 2)]

    def give_gx_block(nb):
        return remote(spare(BLOCKS + nb), spare(nb), xs.at[3 + BLOCKS + nb], xr.at[3 + BLOCKS + nb], pc.partner)

    def give_gx(nb):
        spare(BLOCKS + nb)[...] = product(theirs, nb, 1).reshape(2, TOK // 2 // SUBL, SUBL, COL)
        give_gx_block(nb).start()

    def take_gx(nb):
        give_gx_block(nb).wait_recv()

        def add(h, _):
            at = span(h, STEP)
            finish_block(nb, gx, at, product(at, nb, 1) + flat(nb, 2 + h)[...].reshape(STEP, COL))
            return 0

        lax.fori_loop(0, TOK // STEP, add, 0)

    def loop(n, fn):
        def body(i, _):
            fn(i)
            return 0

        lax.fori_loop(0, n, body, 0)

    def at(t, first, fn, last=None):
        @pl.when((t >= first) & (t <= (first if last is None else last)))
        def _():
            with scope(f"task{first}"):
                fn()

    def last_sends():
        g1.mid(2)
        for i in (1, 2):
            g2.end(ring, i)
            g2.start(plane, i)

    def chunk(q):
        return lax.div(q, 3) + 3 * lax.rem(q, 3)

    def hidden_step(q):
        at(q, 2, last_sends)
        at(q, 2, lambda: g1.end(halves, 1))
        at(q, 4, lambda: g2.mid(0))
        at(q, 5, lambda: g1.end(halves, 2))
        at(q, 7, lambda: g2.mid(1))
        with scope("hidden"):
            chunk_steps(STEPS, hidden_dot, hidden_act, chunk(q), chunk(jnp.minimum(q + 1, CHUNKS - 1)))

    with scope("arrive"):
        g1.end(halves, 0)
    hidden_dot(0, 0)
    loop(CHUNKS, hidden_step)
    loads[3].wait()
    swaps[2].wait_recv()

    def finish(u, tot):
        @pl.when(u < U2)
        def _():
            dw2o[span(lax.rem(u, R), SUBL), span(lax.div(u, R), COL)] = tot

        @pl.when(u >= U2)
        def _():
            v = u - U2
            q = lax.div(v, 2)

            @pl.when(lax.rem(v, 2) == s)
            def _():
                dw1o[:, pl.ds(pl.multiple_of(HALF * s + COL * q, COL), COL)] = tot

            @pl.when(lax.rem(v, 2) != s)
            def _():
                dw1s[:, span(q, COL)] = tot

    rs = Scatter(pc, pool, [recv[:2], recv[2:4], (None, recv[4]), recv[5:]], (rs_s, rs_r), credit, finish)

    def first_dot():
        kept(2 * BLOCKS - 3)
        dhidden_dot(0, 0)
        kept(2 * BLOCKS - 2)

    def dhidden(c):
        chunk_steps(2, dhidden_dot, dhidden_act, c, jnp.minimum(c + 1, CHUNKS - 1))
        grad1(c)

    def settle():
        for i in range(3):
            g2.end(halves, i)
        g1.drain()
        g2.drain()

    def slot(t, come):
        with scope("ev"):
            come = (*rs.events(t, come[:-2]), *come[-2:])

        at(t, 0, lambda: grad2(t), Y_SLOT - 1)
        at(t, 0, lambda: g2.mid(2))
        at(t, Y_SLOT, settle)
        at(t, Y_SLOT, lambda: loop(2, lambda i: give_y(2 * (t - Y_SLOT) + i)), DH_SLOT - 1)
        at(t, DH_SLOT, first_dot)
        at(t, DH_SLOT, lambda: dhidden(t - DH_SLOT), DH_SLOT + CHUNKS - 1)
        at(t, DH_SLOT + 1, lambda: kept(2 * BLOCKS - 1))
        at(t, DH_SLOT + R, lambda: pl.semaphore_signal(spare_sem, inc=1, device_id=pc.partner, device_id_type=MESH))
        at(t, GIVE_SLOTS[0], lambda: pl.semaphore_wait(spare_sem, 1))

        def tokens(nb):
            fetch_y(nb)
            give_gx(nb)
            take_y(nb)

        *come, given, taken = come
        for slots, task, done in ((GIVE_SLOTS, tokens, given), (TAKE_SLOTS, take_gx, taken)):
            come.append(done + how_many(slots, t))
            pl.when(come[-1] > done)(lambda: task(done))
        return tuple(come)

    lax.fori_loop(0, LAST_SLOT + 1, slot, (jnp.int32(0),) * (len(PLAN) + 2))

    with scope("last"):
        last = remote(dw1s, dw1o.at[:, my_lanes], xs.at[11], xr.at[11], pc.partner)
        last.start()
        for c in swaps:
            c.wait_send()
        for nb in range(BLOCKS):
            give_y_block(nb).wait_send()
            give_gx_block(nb).wait_send()
        last.wait()


def copy_out(*refs):
    n = len(refs) // 2
    copies = [pltpu.make_async_copy(src, dst, refs[-1].at[i]) for i, (src, dst) in enumerate(zip(refs[:n], refs[n:]))]
    for c in copies:
        c.start()
    for c in copies:
        c.wait()


def local_stack(x, up, down, g):
    shape = jax.ShapeDtypeStruct
    dma = pltpu.SemaphoreType.DMA
    bf = [(TOK, DIM), (DIM, 2 * TOK), (TOK, DIM), (2, R, R, R, SUBL, HALF), (R, R, R, HALF // R**3, DIM), (2 * TOK, HALF)]
    ff = [(3 * U2, R, R, R, SUBL, COL), (3, TOK, COL), (SUBL, HALF)] + recv_shapes()
    results = [(x.shape, bf16), (g.shape, bf16), (up.shape[1:], f32), (down.shape[1:], f32)]
    res = pl.pallas_call(
        kernel,
        out_shape=[pltpu.VMEM(*q) for q in results] + [shape((n, TOK, COL), f32) for n in (BLOCKS, 2 * BLOCKS)],
        in_specs=[ANY] * 4,
        out_specs=[VMEM] * 4 + [ANY] * 2,
        scratch_shapes=[pltpu.VMEM(q, bf16) for q in bf] + [pltpu.VMEM(q, f32) for q in ff]
        + [dma((n,)) for n in (AG1 + AG2, AG1 + AG2, 6 * SENDS, 4 * sum(SLOTS), 7, 12, 12)]
        + [pltpu.SemaphoreType.REGULAR, pltpu.SemaphoreType.REGULAR((6,))],
        compiler_params=pltpu.CompilerParams(collective_id=0, has_side_effects=True, vmem_limit_bytes=62586880),
        name="stack",
    )(x, up[0], down[0], g)[:4]
    y, gx, dw1, dw2 = pl.pallas_call(
        copy_out,
        out_shape=[shape(*q) for q in results],
        in_specs=[VMEM] * 4,
        out_specs=[ANY] * 4,
        scratch_shapes=[dma((4,))],
        compiler_params=pltpu.CompilerParams(vmem_limit_bytes=2**23),
        name="copy_out",
    )(*res)
    return y, gx, dw1[None], dw2[None]


def solution(mesh):
    tok, mat = P(AXES, None), P(None, AXES, None)
    return jax.shard_map(local_stack, mesh=mesh, in_specs=(tok, mat, mat, tok), out_specs=(tok, tok, mat, mat), check_vma=False)
```

```python
import jax
import jax.numpy as jnp
from jax import lax
from jax.experimental import pallas as pl
from jax.experimental.pallas import tpu as pltpu
from jax.sharding import PartitionSpec as P

f32, bf16 = jnp.float32, jnp.bfloat16
MESH = pl.DeviceIdType.MESH
NN, NT, TN = [(((i,), (k,)), ((), ())) for i, k in ((1, 0), (1, 1), (0, 0))]
ANY = pl.BlockSpec(memory_space=pl.ANY)
VMEM = pl.BlockSpec(memory_space=pltpu.VMEM)
AXES = ("sub", "fsdp")

TOK = 1024
DIM = 1024
HALF = 2048
R = 4
SUBL, LANES = 8, 128
COL = 256
CHUNKS = HALF // COL
STEP = 512
STEPS = 2 * TOK // STEP
DH_BUFFERS = (2, 0)
Y_SLOT, DH_SLOT = 4, 8
U2 = 16
SLOTS = (4, 5, 5)
FEW = 3
SENDS = 4
ROUNDS = (11, 11, 10)
SHORT = 10
CLASSES = DIMS = range(3)
PAIRS = ((0, 1), (2,))
BOTH = range(2)
ORDERS = ((0, 1, 2), (1, 2, 0), (2, 0, 1))
STRIDE = (R * R, R, 1)
C0 = 0.7978845608028654
C1 = 0.044715 * C0
ALL = slice(None)

W1_LANES = ((0, COL, 3), (3 * COL, COL, 3), (6 * COL, COL, 2))
W2_LANES = ((0, LANES, 2), (2 * LANES, LANES, 3), (5 * LANES, LANES, 3))


def dot(a, b, dims):
    return lax.dot_general(a, b, dims, preferred_element_type=f32)


def span(i, n):
    return pl.ds(pl.multiple_of(i * n, n), n)


class Place:
    def __init__(self):
        self.s, self.j = lax.axis_index("sub"), lax.axis_index("fsdp")
        self.c = [lax.rem(lax.div(self.j, n), R) for n in STRIDE]
        self.plus, self.minus, self.opp = [[lax.rem(c + o, R) for c in self.c] for o in (1, 3, 2)]
        self.partner = (1 - self.s, self.j)

    def dev(self, d, v):
        return (self.s, self.j + (v - self.c[d]) * STRIDE[d])

    def near(self, d, dirn):
        return self.minus[d] if dirn else self.plus[d]

    def others(self, d):
        return self.plus[d], self.minus[d], self.opp[d]


def remote(src, dst, ssem, rsem, dev):
    return pltpu.make_async_remote_copy(src, dst, ssem, rsem, device_id=dev, device_id_type=MESH)


def arrived(ref, sem):
    pltpu.make_async_copy(ref, ref, sem).wait()


def part(half):
    return ALL if half is None else pl.ds(2 * half, 2)


class Gather:
    OWN, EARLY, RING, PLANE, HALVES = range(5)

    def __init__(self, pc, w, lead, lanes, sems, base):
        self.pc, self.w, self.lead, self.lanes, self.sems, self.base = pc, w, lead, lanes, sems, base

    @staticmethod
    def count(lanes):
        return 2 + 3 * max(n for _, _, n in lanes)

    def at(self, ln, changes):
        idx = list(self.pc.c)
        for d, v in changes:
            idx[d] = v
        return self.w.at[(*self.lead, *idx, ALL, ln)]

    def classes(self, i):
        return [k for k in CLASSES if i < self.lanes[k][2]]

    def stretch(self, k, step, i):
        lane0, width, subs = self.lanes[k]
        return pl.ds(lane0, width * subs) if step < self.RING else pl.ds(lane0 + i * width, width)

    def sem(self, q, step, i):
        return self.sems[q].at[self.base + step + 3 * i]

    def send(self, block, step, into, i, d, v):
        remote(block, block, self.sem(0, step, i), self.sem(1, into, i), self.pc.dev(d, v)).start()

    def start(self, step, i=0):
        for k in self.classes(i):
            ln = self.stretch(k, step, i)
            d1, d2, d3 = ORDERS[k]
            d = (d1, d2, d2, d3)[step]
            if step < self.RING:
                blocks = [self.at(ln, ())]
            elif step == self.RING:
                blocks = [self.at(ln, ((d1, v),)) for v in self.pc.others(d1)]
            else:
                blocks = [self.at(ln, ((d1, ALL), (d2, ALL)))]
            for v in self.pc.others(d)[:3 if step < self.PLANE else 2]:
                for block in blocks:
                    self.send(block, step, step, i, d, v)

    def mid(self, i=0):
        self.wait(1, self.PLANE, (2, R, R), i)
        for k in self.classes(i):
            d1, d2, d = ORDERS[k]
            for dirn in BOTH:
                behind = self.pc.near(d, 1 - dirn)
                block = self.at(self.stretch(k, self.PLANE, i), ((d1, part(dirn)), (d2, ALL), (d, behind)))
                self.send(block, self.PLANE, self.HALVES, i, d, self.pc.near(d, dirn))

    def wait(self, q, step, box, i):
        lanes = sum(self.lanes[k][1] * (1 if step > self.EARLY else self.lanes[k][2]) for k in self.classes(i))
        arrived(self.w.at[(*self.lead, *[pl.ds(0, m) for m in box], ALL, pl.ds(0, lanes))], self.sem(q, step, i))

    def end(self, step, i=0):
        self.wait(1, step, ((3, 1, 1), (3, 1, 1), (3, 3, 1), None, (1, R, R))[step], i)

    def drain(self):
        for step in (self.OWN, self.EARLY):
            self.wait(0, step, (3, 1, 1), 0)
        for i in range(max(n for _, _, n in self.lanes)):
            self.wait(0, self.RING, (3, 3, 1), i)
            self.wait(0, self.PLANE, (3, R, R), i)


PLAN = (
    ("end", 2, 13, 13233233111),
    ("second_end", 1, 11, 11232252201),
    ("middle", 1, 9, 11221244202),
    ("end", 0, 6, 12203213421),
    ("mid", 0, 4, 11211312313),
    ("start", 0, 2, 11112221221),
)
GIVE_SLOTS = (16, 18, 20, 21)
TAKE_SLOTS = (22, 23, 25, 27)
FIELD = 16


def slots_of(first, later):
    out = [first]
    for digit in str(later)[1:]:
        out.append(out[-1] + int(digit))
    return out


def how_many(slots, t):
    words = [sum(slots.count(FIELD * i + q) << (2 * q) for q in range(FIELD)) for i in range(LAST_SLOT // FIELD + 1)]
    word = jnp.int32(0)
    for i, value in enumerate(words):
        word = jnp.where(lax.div(t, FIELD) == i, jnp.int32(value - (value >> 31 << 32)), word)
    return lax.shift_right_logical(word, 2 * lax.rem(t, FIELD)) & 3


PLAN = [(name, ph, slots_of(*when)) for name, ph, *when in PLAN]
LAST_SLOT = max(q for *_, slots in PLAN for q in slots)


class Scatter:
    def __init__(self, pc, pool, recv, sems, credit, finish):
        self.pc, self.pool, self.recv, self.sems, self.credit, self.finish = pc, pool, recv, sems, credit, finish

    @staticmethod
    def place_of(u):
        v = u - U2
        return jnp.where(u < U2, 2 * U2 + u, R * lax.div(v, 2) + lax.rem(v, 2))

    def blk(self, u, k, ph, v, half):
        order = ORDERS[k]
        idx = [None] * len(order)
        for q in range(ph):
            idx[order[q]] = self.pc.c[order[q]]
        idx[order[ph]] = v
        free = [d for d in DIMS if idx[d] is None]
        for d in free:
            idx[d] = ALL
        if free:
            idx[free[0]] = part(half)
        return self.pool.at[(self.place_of(u), *idx)]

    def landing(self, n, k, ph, dirn, kind, half):
        r = self.recv[ph][kind]
        r = r.at[k, lax.rem(n, r.shape[1]), dirn]
        return r if half is None or not kind else r.at[part(half)]

    def ssem(self, n, pair, ph):
        return self.sems[0].at[(ph * 2 + pair) * SENDS + lax.rem(n, SENDS)]

    def rsem(self, n, pair, ph, kind):
        return self.sems[1].at[4 * sum(SLOTS[:ph]) + (pair * 2 + kind) * SLOTS[ph] + lax.rem(n, SLOTS[ph])]

    def send(self, n, k, ph, src, dst, kind, v):
        pair = k // 2
        remote(src, dst, self.ssem(n, pair, ph), self.rsem(n, pair, ph, kind), self.pc.dev(ORDERS[k][ph], v)).start()

    def copy(self, n, k, ph, dirn, kind):
        d = ORDERS[k][ph]
        near = self.pc.near(d, dirn)
        half = 1 - dirn if kind == 1 else dirn
        src = self.blk(n * 3 + k, k, ph, near if kind else self.pc.opp[d], half)
        dst = self.landing(n, k, ph, dirn, min(kind, 1), half)
        self.send(n, k, ph, src, dst, min(kind, 1), near)

    def start_short(self, n, ks):
        slot = lax.rem(n, SLOTS[1])
        for k in ks:
            slots = [self.recv[1][1].at[k, slot, i] for i in BOTH] + [self.recv[3][0].at[k]]
            for v, dst in zip(self.pc.others(ORDERS[k][1]), slots):
                self.send(n, k, 1, self.blk(n * 3 + k, k, 1, v, None), dst, 1, v)

    def end_short(self, n, ks):
        slot = lax.rem(n, SLOTS[1])
        arrived(self.recv[1][1].at[:, slot], self.rsem(n, 0, 1, 1))
        for k in ks:
            own = self.blk(n * 3 + k, k, 1, self.pc.c[ORDERS[k][1]], None)
            tot = own[...] + self.recv[3][0].at[k][...]
            for i in BOTH:
                tot = tot + self.recv[1][1].at[k, slot, i][...]
            own[...] = tot
        self.sent(n, 0, 1)
        self.start_last(n, ks)

    def received(self, n, pair, ph, kind):
        r, slot = self.recv[ph][kind], 0
        arrived(r.at[2, slot] if pair else r.at[pl.ds(0, 2), slot], self.rsem(n, pair, ph, kind))

    def sent(self, n, pair, ph):
        r = self.recv[ph][1]
        if ph < 2:
            ref = r.at[:, 0, 0] if pair else r.at[:, 0]
        else:
            ref = r.at[2, 0] if pair else r.at[pl.ds(0, 2), 0]
        arrived(ref, self.ssem(n, pair, ph))

    def start(self, n, ks, ph):
        if ph == 0:

            @pl.when(n >= FEW)
            def _():
                for k in ks:
                    for dirn in BOTH:
                        pl.semaphore_wait(self.credit.at[2 * k + dirn], 1)

        for kind in BOTH:
            for k in ks:
                for dirn in BOTH:
                    self.copy(n, k, ph, dirn, kind)

    def give_credit(self, ks):
        for k in ks:
            d = ORDERS[k][0]
            for dirn in BOTH:
                to = self.pc.dev(d, self.pc.near(d, dirn))
                pl.semaphore_signal(self.credit.at[2 * k + 1 - dirn], inc=1, device_id=to, device_id_type=MESH)

    def start_last(self, n, ks):
        for k in ks:
            for i, v in enumerate(self.pc.others(ORDERS[k][2])):
                self.send(n, k, 2, self.blk(n * 3 + k, k, 2, v, None), self.recv[2][1].at[k, lax.rem(n, SLOTS[2]), i], 1, v)

    @staticmethod
    def choose(n, ks, usual, short):
        if len(ks) == 1:
            usual()
        else:
            pl.when(n < SHORT)(usual)
            pl.when(n >= SHORT)(short)

    def middle(self, n, ks, ph):
        self.choose(n, ks, lambda: self.mid(n, ks, ph), lambda: None)

    def second_end(self, n, ks, ph):
        self.choose(n, ks, lambda: self.end(n, ks, ph), lambda: self.end_short(n, ks))

    def mid(self, n, ks, ph):
        self.received(n, ks[0] // 2, ph, 0)
        for k in ks:
            d = ORDERS[k][ph]
            for dirn in BOTH:
                b = self.blk(n * 3 + k, k, ph, self.pc.near(d, dirn), dirn)
                b[...] = b[...] + self.landing(n, k, ph, dirn, 0, None)[...]
        for k in ks:
            for dirn in BOTH:
                self.copy(n, k, ph, dirn, 2)
        if ph == 0:
            pl.when(n == 0)(lambda: self.give_credit(ks))

    def end(self, n, ks, ph):
        self.received(n, ks[0] // 2, ph, 1)
        for k in ks:
            own = self.blk(n * 3 + k, k, ph, self.pc.c[ORDERS[k][ph]], None)
            tot = own[...]
            for i in range(3 if ph == 2 else 2):
                tot = tot + self.recv[ph][1].at[k, lax.rem(n, SLOTS[ph]), i][...]
            if ph < 2:
                own[...] = tot
            else:
                self.finish(n * 3 + k, tot)
        self.sent(n, ks[0] // 2, ph)
        if ph == 0:
            self.choose(n, ks, lambda: self.start(n, ks, 1), lambda: self.start_short(n, ks))

            pl.when(n + SLOTS[0] < ROUNDS[ks[0]])(lambda: self.give_credit(ks))
        elif ph == 1:
            self.start_last(n, ks)

    def events(self, t, come):
        out = []
        for (name, ph, slots), first in zip(PLAN, come):

            def step(n, _):
                for ks in PAIRS:
                    take = lambda: getattr(self, name)(n, ks, ph)
                    pl.when(n < ROUNDS[ks[0]])(take) if ROUNDS[ks[0]] < max(ROUNDS) else take()
                return 0

            out.append(first + how_many(slots, t))
            lax.fori_loop(first, out[-1], step, 0)
        return tuple(out)


def half_tanh(h, h2):
    return 0.5 * jnp.tanh(h * (C0 + C1 * h2))


def gelu(h):
    return h * (0.5 + half_tanh(h, h * h))


def gelu_slope(h):
    h2 = h * h
    t = half_tanh(h, h2)
    return (0.5 + t) + ((0.25 - t * t) * (2.0 * C0 + (6.0 * C1) * h2)) * h


def recv_shapes():
    out = []
    for ph, dims in enumerate(((R, R), (R,))):
        for q in ((2, *dims[1:]), dims):
            out.append((3, SLOTS[ph] if ph or q == dims else FEW, 2, *q, SUBL, COL))
    return out + [(3, SLOTS[2], 3, SUBL, COL), (2, R, SUBL, COL)]


AG1, AG2 = Gather.count(W1_LANES), Gather.count(W2_LANES)
BLOCKS = DIM // COL


def kernel(xh, uph, dnh, gh, y, gx, dw1o, dw2o, landh, keeph, xp, xt, gp, w1, w2, a, pool, sb, dw1s, *rest):
    recv, (ag_s, ag_r, rs_s, rs_r, lsem, xs, xr, spare_sem, credit) = rest[:6], rest[6:]
    pc = Place()
    s = pc.s
    my_lanes, their_lanes = span(s, HALF), span(1 - s, HALF)
    scope = jax.named_scope
    tokens_x, tokens_g = (y, xp), (gx, gp)

    loads = [
        pltpu.make_async_copy(src, dst, lsem.at[i])
        for i, (src, dst) in enumerate((
            (uph.at[:, my_lanes], w1.at[(s, *pc.c)]),
            (dnh, w2.at[tuple(pc.c)]),
            (xh, y),
            (gh, gx),
        ))
    ]
    for c in loads:
        c.start()

    with scope("bar"):
        bar = pltpu.get_barrier_semaphore()
        peers = [pc.partner] + [pc.dev(d, v) for d in DIMS for v in pc.others(d)]
        for dev in peers:
            pl.semaphore_signal(bar, inc=1, device_id=dev, device_id_type=MESH)
        pl.semaphore_wait(bar, len(peers))

    swaps = [
        remote(src, dst, xs.at[i], xr.at[i], pc.partner)
        for i, (src, dst) in enumerate((
            (uph.at[:, their_lanes], w1.at[(s, *pc.c)]),
            (xh, xp),
            (gh, gp),
        ))
    ]
    for c in swaps:
        c.start()

    g1 = Gather(pc, w1, (ALL,), W1_LANES, (ag_s, ag_r), 0)
    g2 = Gather(pc, w2, (), W2_LANES, (ag_s, ag_r), AG1)

    w1f = w1.reshape(DIM, HALF)
    w2f = w2.reshape(HALF, DIM)
    units = pool.reshape(3 * U2, R * R * R, SUBL, COL)

    with scope("swapw"):
        loads[0].wait()
        swaps[0].wait_recv()
    own, early, ring, plane, halves = range(5)
    g1.start(own)
    loads[1].wait()
    g2.start(own)
    g1.start(early)
    g2.start(early)
    with scope("own"):
        g1.end(own)
    for i in range(3):
        g1.start(ring, i)
    with scope("owntwo"):
        g2.end(own)
    for i in range(3):
        g2.start(ring, i)
    with scope("early"):
        g1.end(early)
    for i in BOTH:
        with scope("ring"):
            g1.end(ring, i)
        g1.start(plane, i)
    with scope("mid"):
        g1.mid(0)
    with scope("ring"):
        g1.end(ring, 2)
    g1.start(plane, 2)
    with scope("mid"):
        g1.mid(1)
    with scope("ringtwo"):
        g2.end(early)
        g2.end(ring, 0)
    g2.start(plane, 0)
    def turn(i, _):
        for q, part_x in enumerate(tokens_x):
            xt[:, pl.ds(pl.multiple_of(q * TOK + i * COL, COL), COL)] = part_x[span(i, COL), :].T
        return 0

    loads[2].wait()
    swaps[1].wait_recv()
    with scope("turn"):
        lax.fori_loop(0, TOK // COL, turn, 0)

    def rows(i):
        return slice(STEP * i, STEP * (i + 1))

    def step_of(pair, i):
        return pair[i // 2][rows(i % 2), :]

    def flat(c, i):
        return units.at[R * c + i]

    def hidden_dot(c, i):
        sb[i % 2, :STEP] = dot(step_of(tokens_x, i), w1f[:, span(c, COL)], NN)

    def hidden_act(c, i):
        h = sb[i % 2, :STEP]
        flat(c, i)[...] = h.reshape(STEP // SUBL, SUBL, COL)
        a[rows(i), span(c, COL)] = gelu(h).astype(bf16)

    def dhidden_dot(c, i):
        sb[DH_BUFFERS[i]] = dot(tokens_g[i][...], w2f[span(c, COL), :], NT)

    def dhidden_act(c, i):
        for h in BOTH:
            slope = gelu_slope(flat(c, 2 * i + h)[...].reshape(STEP, COL))
            a[rows(2 * i + h), span(c, COL)] = (slope * sb[DH_BUFFERS[i], rows(h)]).astype(bf16)

    def grad1(c):
        r = dot(xt[...], a[:, span(c, COL)], NN)
        for p in BOTH:
            flat(c, p)[...] = r[rows(p)].reshape(STEP // SUBL, SUBL, COL)

    def chunk_steps(steps, dot_step, act_step, c, after):
        for i in range(steps):
            if i + 1 < steps:
                dot_step(c, i + 1)
            else:
                dot_step(after, 0)
            act_step(c, i)

    def grad2(b):
        both = jnp.concatenate([q[:, span(b, COL)] for q in tokens_g])
        for c in range(CHUNKS):
            r = dot(a[:, COL * c:COL * (c + 1)], both, TN).reshape(SUBL, R, SUBL, COL)
            for q in range(R):
                units[2 * U2 + R * b + q, SUBL * c:SUBL * (c + 1)] = r[:, q]

    own, theirs = pl.ds(0, TOK), pl.ds(TOK, TOK)

    def product(at, nb, i):
        lanes = span(nb, COL)
        return dot(a[at, :], w1f[lanes, :], NT) if i else dot(a[at, :], w2f[:, lanes], NN)

    def keep_y(n):
        return pltpu.make_async_copy(sb.at[lax.rem(n, 3)], keeph.at[n], lsem.at[R + lax.rem(n, 3)])

    def give_y_block(nb):
        return remote(keeph.at[2 * nb], landh.at[nb], xs.at[3 + nb], xr.at[3 + nb], pc.partner)

    def kept(n):
        keep_y(n).wait()

        @pl.when(lax.rem(n, 2) == 0)
        def _():
            give_y_block(lax.div(n, 2)).start()

    def give_y(n):
        @pl.when(n > 2)
        def _():
            kept(n - 3)

        at = span(1 - lax.rem(n, 2), TOK)
        sb[lax.rem(n, 3)] = product(at, lax.div(n, 2), 0)
        keep_y(n).start()

    def finish_block(nb, res, at, part_sum):
        lanes = span(nb, COL)
        res[at, lanes] = (res[at, lanes].astype(f32) + part_sum).astype(bf16)

    def fetched_y(nb):
        return [pltpu.make_async_copy(src, sb.at[b], lsem.at[R + b]) for b, src in enumerate((landh.at[nb], keeph.at[2 * nb + 1]))]

    def fetch_y(nb):
        give_y_block(nb).wait_recv()
        for c in fetched_y(nb):
            c.start()

    def take_y(nb):
        for c in fetched_y(nb):
            c.wait()

        def add(h, _):
            finish_block(nb, y, span(h, COL), sb[0, span(h, COL)] + sb[1, span(h, COL)])
            return 0

        lax.fori_loop(0, TOK // COL, add, 0)

    def spare(n):
        return units.at[pl.ds(R * n + 2, 2)]

    def give_gx_block(nb):
        return remote(spare(BLOCKS + nb), spare(nb), xs.at[3 + BLOCKS + nb], xr.at[3 + BLOCKS + nb], pc.partner)

    def give_gx(nb):
        spare(BLOCKS + nb)[...] = product(theirs, nb, 1).reshape(2, TOK // 2 // SUBL, SUBL, COL)
        give_gx_block(nb).start()

    def take_gx(nb):
        give_gx_block(nb).wait_recv()

        def add(h, _):
            at = span(h, STEP)
            finish_block(nb, gx, at, product(at, nb, 1) + flat(nb, 2 + h)[...].reshape(STEP, COL))
            return 0

        lax.fori_loop(0, TOK // STEP, add, 0)

    def loop(n, fn):
        def body(i, _):
            fn(i)
            return 0

        lax.fori_loop(0, n, body, 0)

    def at(t, first, fn, last=None):
        @pl.when((t >= first) & (t <= (first if last is None else last)))
        def _():
            with scope(f"task{first}"):
                fn()

    def last_sends():
        g1.mid(2)
        for i in (1, 2):
            g2.end(ring, i)
            g2.start(plane, i)

    def chunk(q):
        return lax.div(q, 3) + 3 * lax.rem(q, 3)

    def hidden_step(q):
        at(q, 2, last_sends)
        at(q, 2, lambda: g1.end(halves, 1))
        at(q, 4, lambda: g2.mid(0))
        at(q, 5, lambda: g1.end(halves, 2))
        at(q, 7, lambda: g2.mid(1))
        with scope("hidden"):
            chunk_steps(STEPS, hidden_dot, hidden_act, chunk(q), chunk(jnp.minimum(q + 1, CHUNKS - 1)))

    with scope("arrive"):
        g1.end(halves, 0)
    hidden_dot(0, 0)
    loop(CHUNKS, hidden_step)
    loads[3].wait()
    swaps[2].wait_recv()

    def finish(u, tot):
        @pl.when(u < U2)
        def _():
            dw2o[span(lax.rem(u, R), SUBL), span(lax.div(u, R), COL)] = tot

        @pl.when(u >= U2)
        def _():
            v = u - U2
            q = lax.div(v, 2)

            @pl.when(lax.rem(v, 2) == s)
            def _():
                dw1o[:, pl.ds(pl.multiple_of(HALF * s + COL * q, COL), COL)] = tot

            @pl.when(lax.rem(v, 2) != s)
            def _():
                dw1s[:, span(q, COL)] = tot

    rs = Scatter(pc, pool, [recv[:2], recv[2:4], (None, recv[4]), recv[5:]], (rs_s, rs_r), credit, finish)

    def first_dot():
        kept(2 * BLOCKS - 3)
        dhidden_dot(0, 0)
        kept(2 * BLOCKS - 2)

    def dhidden(c):
        chunk_steps(2, dhidden_dot, dhidden_act, c, jnp.minimum(c + 1, CHUNKS - 1))
        grad1(c)

    def settle():
        for i in range(3):
            g2.end(halves, i)

    def slot(t, come):
        with scope("ev"):
            come = (*rs.events(t, come[:-2]), *come[-2:])

        at(t, 0, lambda: grad2(t), Y_SLOT - 1)
        at(t, 0, lambda: g2.mid(2))
        at(t, Y_SLOT, settle)
        at(t, Y_SLOT, lambda: loop(2, lambda i: give_y(2 * (t - Y_SLOT) + i)), DH_SLOT - 1)
        at(t, DH_SLOT, first_dot)
        at(t, DH_SLOT, lambda: dhidden(t - DH_SLOT), DH_SLOT + CHUNKS - 1)
        at(t, DH_SLOT + 1, lambda: kept(2 * BLOCKS - 1))
        at(t, DH_SLOT + R, lambda: pl.semaphore_signal(spare_sem, inc=1, device_id=pc.partner, device_id_type=MESH))
        at(t, GIVE_SLOTS[0] + 1, g1.drain)
        at(t, GIVE_SLOTS[0] + 1, g2.drain)
        at(t, GIVE_SLOTS[0], lambda: pl.semaphore_wait(spare_sem, 1))

        def tokens(nb):
            fetch_y(nb)
            give_gx(nb)
            take_y(nb)

        *come, given, taken = come
        for slots, task, done in ((GIVE_SLOTS, tokens, given), (TAKE_SLOTS, take_gx, taken)):
            come.append(done + how_many(slots, t))
            pl.when(come[-1] > done)(lambda: task(done))
        return tuple(come)

    lax.fori_loop(0, LAST_SLOT + 1, slot, (jnp.int32(0),) * (len(PLAN) + 2))

    with scope("last"):
        last = remote(dw1s, dw1o.at[:, my_lanes], xs.at[11], xr.at[11], pc.partner)
        last.start()
        for c in swaps:
            c.wait_send()
        for nb in range(BLOCKS):
            give_y_block(nb).wait_send()
            give_gx_block(nb).wait_send()
        last.wait()


def copy_out(*refs):
    n = len(refs) // 2
    copies = [pltpu.make_async_copy(src, dst, refs[-1].at[i]) for i, (src, dst) in enumerate(zip(refs[:n], refs[n:]))]
    for c in copies:
        c.start()
    for c in copies:
        c.wait()


def local_stack(x, up, down, g):
    shape = jax.ShapeDtypeStruct
    dma = pltpu.SemaphoreType.DMA
    bf = [(TOK, DIM), (DIM, 2 * TOK), (TOK, DIM), (2, R, R, R, SUBL, HALF), (R, R, R, HALF // R**3, DIM), (2 * TOK, HALF)]
    ff = [(3 * U2, R, R, R, SUBL, COL), (3, TOK, COL), (SUBL, HALF)] + recv_shapes()
    results = [(x.shape, bf16), (g.shape, bf16), (up.shape[1:], f32), (down.shape[1:], f32)]
    res = pl.pallas_call(
        kernel,
        out_shape=[pltpu.VMEM(*q) for q in results] + [shape((n, TOK, COL), f32) for n in (BLOCKS, 2 * BLOCKS)],
        in_specs=[ANY] * 4,
        out_specs=[VMEM] * 4 + [ANY] * 2,
        scratch_shapes=[pltpu.VMEM(q, bf16) for q in bf] + [pltpu.VMEM(q, f32) for q in ff]
        + [dma((n,)) for n in (AG1 + AG2, AG1 + AG2, 6 * SENDS, 4 * sum(SLOTS), 7, 12, 12)]
        + [pltpu.SemaphoreType.REGULAR, pltpu.SemaphoreType.REGULAR((6,))],
        compiler_params=pltpu.CompilerParams(collective_id=0, has_side_effects=True, vmem_limit_bytes=62586880),
        name="stack",
    )(x, up[0], down[0], g)[:4]
    y, gx, dw1, dw2 = pl.pallas_call(
        copy_out,
        out_shape=[shape(*q) for q in results],
        in_specs=[VMEM] * 4,
        out_specs=[ANY] * 4,
        scratch_shapes=[dma((4,))],
        compiler_params=pltpu.CompilerParams(vmem_limit_bytes=2**23),
        name="copy_out",
    )(*res)
    return y, gx, dw1[None], dw2[None]


def solution(mesh):
    tok, mat = P(AXES, None), P(None, AXES, None)
    return jax.shard_map(local_stack, mesh=mesh, in_specs=(tok, mat, mat, tok), out_specs=(tok, tok, mat, mat), check_vma=False)
```
